512 devices in a mesh: row: 64 (over y, x, core), col: 8 (over z).
Axes of the slice: x: 4, y: 8, z: 8, core: 2. Of those that a mesh axis runs over, the one named last changes fastest.
Arguments:
- matrix: float32 [32768, 4096], P('row', 'col'), may hold values from -6 to 6
- first_leaves: float32 [32768, 256], P('row', 'col'), may hold values from -0.25 to 0.25
- first_factors: float32 [16384, 256], P('row', 'col'), may hold values from -0.1875 to 0.1875
- first_merges: float32 [16384, 256], P('row', 'col'), may hold values from -0.375 to 0.375
- first_mixers: float32 [16384, 256], P('row', 'col'), may hold values from -0.1875 to 0.1875
- second_leaves: float32 [32768, 256], P('row', 'col'), may hold values from -0.25 to 0.25
- second_factors: float32 [16384, 256], P('row', 'col'), may hold values from -0.1875 to 0.1875
- second_merges: float32 [16384, 256], P('row', 'col'), may hold values from -0.375 to 0.375
- second_mixers: float32 [16384, 256], P('row', 'col'), may hold values from -0.1875 to 0.1875
Outputs:
- updated: float32 [32768, 4096], P('row', 'col')
The draws below stay inside these ranges and needn't reach their ends.
All inputs are finite; a program needn't handle non-finite values.
Results may differ from the reference program's by a relative error of at most 0.0001.
Values sent between devices are 32-bit elements; how exact they have to be, the bound alone decides.
A program may use at most 64 MiB of HBM per device.

```python
import jax
import jax.numpy as jnp
from jax import lax

B = 256
ROWS_DEV = 512
LEVELS = 6
ROWS = 32768
COLS = 4096
N_ROW = 64


def block_levels(rng, dims, cuts, least, largest):
    def one(position, blocks):
        steps = jax.random.uniform(jax.random.fold_in(jax.random.fold_in(rng, 6), position), (blocks,), jnp.float32, least / len(cuts), largest / len(cuts))
        return jnp.repeat(jnp.exp(steps), dims[position] // blocks).reshape((-1,) + (1,) * (len(dims) - position - 1))

    factor_of = one(*cuts[0])
    for cut in cuts[1:]:
        factor_of = factor_of * one(*cut)
    return factor_of


def normal_values(rng, extent, spread, limit, pieces=(), held_as=jnp.bfloat16):
    values = spread * jax.random.normal(rng, extent, jnp.float32)
    if pieces:
        values = values * block_levels(rng, extent, pieces, -0.22, 0.18)
    return jnp.clip(values, -limit, limit).astype(held_as)


def setup_inputs(seed: int = 0) -> dict:
    key_of = jax.random.split(jax.random.key(seed), 10)
    return {
        "matrix": normal_values(key_of[0], (ROWS, COLS), 1.0, 6.0, ((0, 64), (1, 8)), jnp.float32),
        "first_leaves": normal_values(key_of[1], (ROWS, B), ROWS_DEV ** -0.5, 0.25, ((0, 64), (1, 8)), jnp.float32),
        "first_factors": normal_values(key_of[2], (N_ROW * B, B), (4 * B) ** -0.5, 0.1875, ((0, 64), (1, 8)), jnp.float32),
        "first_merges": normal_values(key_of[3], (N_ROW * B, B), B ** -0.5, 0.375, ((0, 64), (1, 8)), jnp.float32),
        "first_mixers": normal_values(key_of[4], (N_ROW * B, B), (4 * B) ** -0.5, 0.1875, ((0, 64), (1, 8)), jnp.float32),
        "second_leaves": normal_values(key_of[5], (ROWS, B), ROWS_DEV ** -0.5, 0.25, ((0, 64), (1, 8)), jnp.float32),
        "second_factors": normal_values(key_of[6], (N_ROW * B, B), (4 * B) ** -0.5, 0.1875, ((0, 64), (1, 8)), jnp.float32),
        "second_merges": normal_values(key_of[7], (N_ROW * B, B), B ** -0.5, 0.375, ((0, 64), (1, 8)), jnp.float32),
        "second_mixers": normal_values(key_of[8], (N_ROW * B, B), (4 * B) ** -0.5, 0.1875, ((0, 64), (1, 8)), jnp.float32),
    }


def product(left, right):
    return jnp.dot(left, right, precision=lax.Precision.HIGHEST)


def leaf_vectors(supplied, offset):
    row_index = jnp.arange(supplied.shape[0], dtype=jnp.int32)[:, None] - offset
    col_index = jnp.arange(supplied.shape[1], dtype=jnp.int32)[None, :]
    unit = jnp.where(row_index == col_index, 1.0, 0.0).astype(supplied.dtype)
    return jnp.where(row_index > col_index, supplied, unit)


def reference(matrix, first_leaves, first_factors, first_merges, first_mixers, second_leaves, second_factors, second_merges, second_mixers):
    blocks = [matrix[owner * ROWS_DEV:(owner + 1) * ROWS_DEV] for owner in range(N_ROW)]
    panels = [(first_leaves, first_factors, first_merges, first_mixers), (second_leaves, second_factors, second_merges, second_mixers)]
    for panel_index in range(2):
        leaves, factors, merges, mixers = panels[panel_index]
        offsets = [B if (panel_index == 1 and owner == 0) else 0 for owner in range(N_ROW)]
        for owner in range(N_ROW):
            vectors = leaf_vectors(leaves[owner * ROWS_DEV:(owner + 1) * ROWS_DEV], offsets[owner])
            factor = jnp.triu(factors[owner * B:(owner + 1) * B])
            blocks[owner] = blocks[owner] - product(vectors, product(factor.T, product(vectors.T, blocks[owner])))
        for level_index in range(LEVELS):
            stride = 2 ** level_index
            for owner in range(0, N_ROW, 2 * stride):
                partner = owner + stride
                merge = jnp.triu(merges[partner * B:(partner + 1) * B])
                mixer = jnp.triu(mixers[partner * B:(partner + 1) * B])
                start = offsets[owner]
                upper_rows = blocks[owner][start:start + B]
                lower_rows = blocks[partner][:B]
                weight = product(mixer.T, upper_rows + product(merge.T, lower_rows))
                blocks[owner] = blocks[owner].at[start:start + B].set(upper_rows - weight)
                blocks[partner] = blocks[partner].at[:B].set(lower_rows - product(merge, weight))
    return jnp.concatenate(blocks, 0)
```

```python
import functools

import jax
import jax.numpy as jnp
from jax import lax
from jax.experimental import pallas as pl
from jax.experimental.pallas import tpu as pltpu
from jax.sharding import PartitionSpec as P

LANES = 128
MESH = pl.DeviceIdType.MESH
F32 = jnp.float32
BF16 = jnp.bfloat16


def halves(value):
    high = value.astype(BF16)
    return high, (value - high.astype(F32)).astype(BF16)


def left_operand(value):
    high, low = halves(value)
    return jnp.concatenate([high, high, low], axis=1)


def times(operator, value):
    high, low = halves(value)
    right = jnp.concatenate([high, low, high], axis=0)
    return jnp.dot(operator[...], right, preferred_element_type=F32)


def lower_triangle(value):
    row = lax.broadcasted_iota(jnp.int32, value.shape, 0)
    col = lax.broadcasted_iota(jnp.int32, value.shape, 1)
    return jnp.where(col <= row, value, 0.0)


def kernel(
    levels,
    ring_size,
    matrix,
    v1,
    f1,
    u1,
    g1,
    v2,
    f2,
    u2,
    g2,
    out,
    x,
    leafs,
    trees,
    far_mixers,
    tops,
    far_folds,
    folds,
    far_tops,
    op_v,
    op_vt,
    op_f,
    op_u,
    op_ut,
    op_g,
    op_far,
    load_sem,
    x_sem,
    out_sem,
    ring_send,
    ring_recv,
    fold_send,
    fold_recv,
    top_send,
    top_recv,
    mixer_send,
    mixer_recv,
):
    chunks, rows, _ = x.shape
    width = trees.shape[1]
    share = width // ring_size
    half = ring_size // 2

    d = lax.axis_index("row")
    k = lax.axis_index("col")
    right = lax.rem(k + 1, ring_size)
    left = lax.rem(k + ring_size - 1, ring_size)
    steps = jnp.int32(0)
    reach = jnp.int32(1)
    for i in range(levels):
        one = jnp.where(lax.rem(d, 2 ** (i + 1)) == 0, 1, 0)
        steps = steps + one
        reach = reach + one * 2**i
    not_root = d != 0
    parent = d - reach

    own = pl.ds(pl.multiple_of(k * share, share), share)
    loads = []
    for p, (v, f, u, g) in enumerate(((v1, f1, u1, g1), (v2, f2, u2, g2))):
        places = (
            (v, leafs.at[p, own, pl.ds(0, rows)]),
            (f, leafs.at[p, own, pl.ds(rows, width)]),
            (u, trees.at[p, own, pl.ds(0, width)]),
            (g, trees.at[p, own, pl.ds(width, width)]),
        )
        for i, (source, place) in enumerate(places):
            loads.append(pltpu.make_async_copy(source, place, load_sem.at[p, i]))
    x_loads = [
        pltpu.make_async_copy(
            matrix.at[:, pl.ds(c * LANES, LANES)], x.at[c], x_sem.at[c]
        )
        for c in range(chunks)
    ]
    for copy in loads[:4] + x_loads + loads[4:]:
        copy.start()

    barrier = pltpu.get_barrier_semaphore()

    def greet(row, col):
        pl.semaphore_signal(barrier, inc=1, device_id=(row, col), device_id_type=MESH)

    greet(d, left)
    greet(d, right)

    def greet_lower(i, stride):
        greet(d + stride, k)
        return stride * 2

    lax.fori_loop(0, steps, greet_lower, jnp.int32(1))

    @pl.when(not_root)
    def _():
        greet(parent, k)

    pl.semaphore_wait(barrier, 2 + steps + jnp.where(not_root, 1, 0))

    def hops(piece, way):
        return half if piece == way else half - 1

    def ring_copy(p, piece, way, hop, sent):
        back = hop - 1 if sent else hop
        shard = lax.rem(k + (ring_size - back if way == 0 else back), ring_size)
        row = pl.ds(pl.multiple_of(shard * share, share), share)
        if piece == 0:
            first = pl.multiple_of(((shard * share) // LANES) * LANES, LANES)
            ref = leafs.at[p, row, pl.ds(first, rows + LANES)]
        else:
            ref = trees.at[p, row, :]
        return pltpu.make_async_remote_copy(
            src_ref=ref,
            dst_ref=ref,
            send_sem=ring_send.at[p, piece, way, hop - 1],
            recv_sem=ring_recv.at[p, piece, way, hop - 1],
            device_id=(d, right if way == 0 else left),
            device_id_type=MESH,
        )

    def relay(p, hop):
        for piece in range(2):
            for way in range(2):
                if hop <= hops(piece, way):
                    if hop > 1:
                        ring_copy(p, piece, way, hop - 1, False).wait_recv()
                    ring_copy(p, piece, way, hop, True).start()

    def gathered(p, piece):
        for way in range(2):
            if hops(piece, way) > 0:
                ring_copy(p, piece, way, hops(piece, way), False).wait_recv()

    def top_copy(p, level, c, stride):
        return pltpu.make_async_remote_copy(
            src_ref=tops.at[p, level, c],
            dst_ref=far_tops.at[p, c],
            send_sem=top_send.at[p, level, c],
            recv_sem=top_recv.at[p, c],
            device_id=(d + stride, k),
            device_id_type=MESH,
        )

    def fold_copy(p, c, level):
        return pltpu.make_async_remote_copy(
            src_ref=folds.at[p, c],
            dst_ref=far_folds.at[p, level, c],
            send_sem=fold_send.at[p, c],
            recv_sem=fold_recv.at[p, level, c],
            device_id=(parent, k),
            device_id_type=MESH,
        )

    def mixer_copy(p, level):
        return pltpu.make_async_remote_copy(
            src_ref=trees.at[p, :, pl.ds(width, width)],
            dst_ref=far_mixers.at[p, level],
            send_sem=mixer_send.at[p],
            recv_sem=mixer_recv.at[p, level],
            device_id=(parent, k),
            device_id_type=MESH,
        )

    def fold(p, c):
        folds[p, c] = times(op_ut, tops[p, steps, c])
        fold_copy(p, c, steps).start()

    def each_chunk(body):
        def step(c, carry):
            body(c)
            return carry

        lax.fori_loop(0, chunks, step, 0)

    def prepare_leaf(p, offset):
        raw = leafs[p, :, pl.ds(0, rows)]
        row = lax.broadcasted_iota(jnp.int32, raw.shape, 1) - offset
        col = lax.broadcasted_iota(jnp.int32, raw.shape, 0)
        vectors = jnp.where(row > col, raw, jnp.where(row == col, 1.0, 0.0))
        op_vt[...] = left_operand(vectors)
        op_v[...] = left_operand(vectors.T)
        op_f[...] = left_operand(lower_triangle(leafs[p, :, pl.ds(rows, width)]))

    def prepare_tree(p):
        merge = lower_triangle(trees[p, :, pl.ds(0, width)])
        op_ut[...] = left_operand(merge)
        op_u[...] = left_operand(merge.T)
        op_g[...] = left_operand(lower_triangle(trees[p, :, pl.ds(width, width)]))

    def panel(p, offset):
        block = pl.ds(pl.multiple_of(offset, width), width)
        gathered(p, 0)
        prepare_leaf(p, offset)
        if p == 0:
            for copy in x_loads:
                copy.wait()

        def leaf(c):
            before = x[c]
            mixed = times(op_f, times(op_vt, before))
            x[c] = before - times(op_v, mixed)
            tops[p, 0, c] = x[c, block, :]

            @pl.when(steps > 0)
            def _():
                top_copy(p, 0, c, 1).start()

        each_chunk(leaf)
        gathered(p, 1)

        @pl.when(not_root)
        def _():
            mixer_copy(p, steps).start()

        prepare_tree(p)

        @pl.when(steps == 0)
        def _():
            each_chunk(functools.partial(fold, p))

        def level_step(level, stride):
            mixer_copy(p, level).wait_recv()
            op_far[...] = left_operand(lower_triangle(far_mixers[p, level]))

            def upper(c):
                fold_copy(p, c, level).wait_recv()
                before = tops[p, level, c]
                weight = times(op_far, before + far_folds[p, level, c])
                tops[p, level + 1, c] = before - weight

                @pl.when(level + 1 < steps)
                def _():
                    top_copy(p, level + 1, c, stride * 2).start()

                @pl.when((level + 1 == steps) & not_root)
                def _():
                    fold(p, c)

            each_chunk(upper)
            if p == 0:
                for hop in range(2, half + 1):

                    @pl.when(level == hop - 2)
                    def _():
                        relay(1, hop)

            return stride * 2

        lax.fori_loop(0, steps, level_step, jnp.int32(1))

        def lower(c):
            top_copy(p, 0, c, 0).wait_recv()
            weight = times(op_g, far_tops[p, c] + folds[p, c])
            x[c, pl.ds(0, width), :] = tops[p, steps, c] - times(op_u, weight)

        def root(c):
            x[c, block, :] = tops[p, levels, c]

        @pl.when(not_root)
        def _():
            each_chunk(lower)

        @pl.when(d == 0)
        def _():
            each_chunk(root)

        if p == 0:
            for hop in range(2, half + 1):

                @pl.when(steps <= hop - 2)
                def _():
                    relay(1, hop)

    for copy in loads[:4]:
        copy.wait()
    for hop in range(1, half + 1):
        relay(0, hop)
    for copy in loads[4:]:
        copy.wait()
    relay(1, 1)
    panel(0, jnp.int32(0))
    panel(1, jnp.where(d == 0, width, 0))

    stores = [
        pltpu.make_async_copy(
            x.at[c], out.at[:, pl.ds(c * LANES, LANES)], out_sem.at[c]
        )
        for c in range(chunks)
    ]
    for copy in stores:
        copy.start()

    for p in range(2):
        for piece in range(2):
            for way in range(2):
                for hop in range(1, hops(piece, way) + 1):
                    ring_copy(p, piece, way, hop, True).wait_send()

        def sent_tops(level, carry):
            each_chunk(lambda c: top_copy(p, level, c, 0).wait_send())
            return carry

        lax.fori_loop(0, steps, sent_tops, 0)

        @pl.when(not_root)
        def _():
            mixer_copy(p, steps).wait_send()
            each_chunk(lambda c: fold_copy(p, c, steps).wait_send())

    for copy in stores:
        copy.wait()


def local(levels, ring_size, matrix, *reflectors):
    rows, cols = matrix.shape
    turned = [r.T for r in reflectors]
    width = turned[1].shape[1]
    chunks = cols // LANES
    half = ring_size // 2
    vmem, dma = pltpu.VMEM, pltpu.SemaphoreType.DMA
    anywhere = pl.BlockSpec(memory_space=pl.ANY)
    tile = (chunks, width, LANES)
    flops = 2 * 3 * 2 * cols * width * (3 * rows + 9 * width)
    return pl.pallas_call(
        functools.partial(kernel, levels, ring_size),
        out_shape=jax.ShapeDtypeStruct(matrix.shape, matrix.dtype),
        in_specs=[anywhere] * 9,
        out_specs=anywhere,
        scratch_shapes=[
            vmem((chunks, rows, LANES), F32),
            vmem((2, width, rows + width), F32),
            vmem((2, width, 2 * width), F32),
            vmem((2, levels, width, width), F32),
            vmem((2, levels + 1, *tile), F32),
            vmem((2, levels, *tile), F32),
            vmem((2, *tile), F32),
            vmem((2, *tile), F32),
            vmem((rows, 3 * width), BF16),
            vmem((width, 3 * rows), BF16),
            vmem((width, 3 * width), BF16),
            vmem((width, 3 * width), BF16),
            vmem((width, 3 * width), BF16),
            vmem((width, 3 * width), BF16),
            vmem((width, 3 * width), BF16),
            dma((2, 4)),
            dma((chunks,)),
            dma((chunks,)),
            dma((2, 2, 2, half)),
            dma((2, 2, 2, half)),
            dma((2, chunks)),
            dma((2, levels, chunks)),
            dma((2, levels, chunks)),
            dma((2, chunks)),
            dma((2,)),
            dma((2, levels)),
        ],
        compiler_params=pltpu.CompilerParams(
            collective_id=0, has_side_effects=True, vmem_limit_bytes=48 * 2**20
        ),
        cost_estimate=pl.CostEstimate(
            flops=flops, bytes_accessed=8 * rows * cols, transcendentals=0
        ),
        name="tree_update",
    )(matrix, *turned)


def solution(mesh):
    levels = mesh.shape["row"].bit_length() - 1
    placed = P("row", "col")
    return jax.shard_map(
        functools.partial(local, levels, mesh.shape["col"]),
        mesh=mesh,
        in_specs=(placed,) * 9,
        out_specs=placed,
        check_vma=False,
    )
```

```python
import functools

import jax
import jax.numpy as jnp
from jax import lax
from jax.experimental import pallas as pl
from jax.experimental.pallas import tpu as pltpu
from jax.sharding import PartitionSpec as P

LANES = 128
PAIR = 256
MESH = pl.DeviceIdType.MESH
F32 = jnp.float32
BF16 = jnp.bfloat16


def halves(value):
    high = value.astype(BF16)
    return high, (value - high.astype(F32)).astype(BF16)


def left_operand(value):
    high, low = halves(value)
    return jnp.concatenate([high, high, low], axis=1)


def times(operator, value):
    high, low = halves(value)
    right = jnp.concatenate([high, low, high], axis=0)
    return jnp.dot(operator[...], right, preferred_element_type=F32)


def lower_triangle(value):
    row = lax.broadcasted_iota(jnp.int32, value.shape, 0)
    col = lax.broadcasted_iota(jnp.int32, value.shape, 1)
    return jnp.where(col <= row, value, 0.0)


def kernel(
    levels,
    ring_size,
    matrix,
    v1,
    f1,
    u1,
    g1,
    v2,
    f2,
    u2,
    g2,
    x,
    leafs,
    trees,
    far_mixers,
    tops,
    far_folds,
    folds,
    far_tops,
    op_v,
    op_vt,
    op_f,
    op_u,
    op_ut,
    op_g,
    op_far,
    load_sem,
    x_sem,
    ring_send,
    ring_recv,
    fold_send,
    fold_recv,
    top_send,
    top_recv,
    mixer_send,
    mixer_recv,
):
    rows, columns = x.shape
    chunks = columns // LANES
    pairs = columns // PAIR
    width = trees.shape[1]
    share = width // ring_size
    half = ring_size // 2

    d = lax.axis_index("row")
    k = lax.axis_index("col")
    right = lax.rem(k + 1, ring_size)
    left = lax.rem(k + ring_size - 1, ring_size)
    steps = jnp.int32(0)
    reach = jnp.int32(1)
    for i in range(levels):
        one = jnp.where(lax.rem(d, 2 ** (i + 1)) == 0, 1, 0)
        steps = steps + one
        reach = reach + one * 2**i
    not_root = d != 0
    parent = d - reach

    own = pl.ds(pl.multiple_of(k * share, share), share)
    loads = []
    for p, (v, f, u, g) in enumerate(((v1, f1, u1, g1), (v2, f2, u2, g2))):
        places = (
            (v, leafs.at[p, own, pl.ds(0, rows)]),
            (f, leafs.at[p, own, pl.ds(rows, width)]),
            (u, trees.at[p, own, pl.ds(0, width)]),
            (g, trees.at[p, own, pl.ds(width, width)]),
        )
        for i, (source, place) in enumerate(places):
            loads.append(pltpu.make_async_copy(source, place, load_sem.at[p, i]))
    x_load = pltpu.make_async_copy(matrix, x, x_sem)

    barrier = pltpu.get_barrier_semaphore()

    def greet(row, col):
        pl.semaphore_signal(barrier, inc=1, device_id=(row, col), device_id_type=MESH)

    greet(d, left)
    greet(d, right)

    def greet_lower(i, stride):
        greet(d + stride, k)
        return stride * 2

    lax.fori_loop(0, steps, greet_lower, jnp.int32(1))

    @pl.when(not_root)
    def _():
        greet(parent, k)

    for copy in loads[:4] + [x_load] + loads[4:]:
        copy.start()
    with jax.named_scope("barrier"):
        pl.semaphore_wait(barrier, 2 + steps + jnp.where(not_root, 1, 0))

    starts = ((0, 2 * LANES), (2 * LANES, rows - LANES), (0, width), (width, width))

    def hops(piece, way):
        return half if piece % 2 == way else half - 1

    def ring_copy(p, piece, way, hop, sent):
        back = hop - 1 if sent else hop
        shard = lax.rem(k + (ring_size - back if way == 0 else back), ring_size)
        row = pl.ds(pl.multiple_of(shard * share, share), share)
        start, size = starts[piece]
        if piece < 2:
            first = ((shard * share) // LANES) * LANES
            lanes = pl.ds(pl.multiple_of(first + start, LANES), size)
            ref = leafs.at[p, row, lanes]
        else:
            ref = trees.at[p, row, pl.ds(start, size)]
        return pltpu.make_async_remote_copy(
            src_ref=ref,
            dst_ref=ref,
            send_sem=ring_send.at[p, piece, way, hop - 1],
            recv_sem=ring_recv.at[p, piece, way, hop - 1],
            device_id=(d, right if way == 0 else left),
            device_id_type=MESH,
        )

    def relay(p, hop):
        for piece in range(4):
            for way in range(2):
                if hop <= hops(piece, way):
                    if hop > 1:
                        ring_copy(p, piece, way, hop - 1, False).wait_recv()
                    ring_copy(p, piece, way, hop, True).start()

    def gathered(p, pieces):
        for piece in pieces:
            for way in range(2):
                if hops(piece, way) > 0:
                    ring_copy(p, piece, way, hops(piece, way), False).wait_recv()

    def top_copy(p, level, c, stride):
        return pltpu.make_async_remote_copy(
            src_ref=tops.at[p, level, c],
            dst_ref=far_tops.at[p, c],
            send_sem=top_send.at[p, level, c],
            recv_sem=top_recv.at[p, c],
            device_id=(d + stride, k),
            device_id_type=MESH,
        )

    def fold_copy(p, c, level):
        return pltpu.make_async_remote_copy(
            src_ref=folds.at[p, c],
            dst_ref=far_folds.at[p, level, c],
            send_sem=fold_send.at[p, c],
            recv_sem=fold_recv.at[p, level, c],
            device_id=(parent, k),
            device_id_type=MESH,
        )

    def mixer_copy(p, level):
        return pltpu.make_async_remote_copy(
            src_ref=trees.at[p, :, pl.ds(width, width)],
            dst_ref=far_mixers.at[p, level],
            send_sem=mixer_send.at[p],
            recv_sem=mixer_recv.at[p, level],
            device_id=(parent, k),
            device_id_type=MESH,
        )

    def fold(p, c):
        folds[p, c] = times(op_ut, tops[p, steps, c])
        fold_copy(p, c, steps).start()

    def chunks_of(pair):
        return range(pair * (PAIR // LANES), (pair + 1) * (PAIR // LANES))

    def each_chunk(body):
        def step(c, carry):
            body(c)
            return carry

        lax.fori_loop(0, chunks, step, 0)

    def prepare_leaf(p, offset):
        raw = leafs[p, :, pl.ds(0, rows)]
        row = lax.broadcasted_iota(jnp.int32, raw.shape, 1) - offset
        col = lax.broadcasted_iota(jnp.int32, raw.shape, 0)
        vectors = jnp.where(row > col, raw, jnp.where(row == col, 1.0, 0.0))
        op_vt[...] = left_operand(vectors)
        op_v[...] = left_operand(vectors.T)
        op_f[...] = left_operand(lower_triangle(leafs[p, :, pl.ds(rows, width)]))

    def prepare_tree(p):
        merge = lower_triangle(trees[p, :, pl.ds(0, width)])
        op_ut[...] = left_operand(merge)
        op_u[...] = left_operand(merge.T)
        op_g[...] = left_operand(lower_triangle(trees[p, :, pl.ds(width, width)]))

    def panel(p, offset):
        block = pl.ds(pl.multiple_of(offset, width), width)
        with jax.named_scope("wait_vectors"):
            gathered(p, (0, 1))
        with jax.named_scope("prepare_leaf"):
            prepare_leaf(p, offset)
        if p == 0:
            x_load.wait()

        with jax.named_scope("leaf"):
            for pair in range(pairs):
                lanes = pl.ds(pair * PAIR, PAIR)
                before = x[:, lanes]
                mixed = times(op_f, times(op_vt, before))
                x[:, lanes] = before - times(op_v, mixed)
                for c in chunks_of(pair):
                    tops[p, 0, c] = x[block, pl.ds(c * LANES, LANES)]

                    @pl.when(steps > 0)
                    def _():
                        top_copy(p, 0, c, 1).start()
        with jax.named_scope("wait_merges"):
            gathered(p, (2, 3))

        @pl.when(not_root)
        def _():
            mixer_copy(p, steps).start()

        with jax.named_scope("prepare_tree"):
            prepare_tree(p)

        @pl.when(steps == 0)
        def _():
            with jax.named_scope("first_fold"):
                each_chunk(functools.partial(fold, p))

        def level_step(level, stride):
            with jax.named_scope("wait_mixer"):
                mixer_copy(p, level).wait_recv()
            op_far[...] = left_operand(lower_triangle(far_mixers[p, level]))

            def upper(c):
                with jax.named_scope("wait_fold"):
                    fold_copy(p, c, level).wait_recv()
                before = tops[p, level, c]
                weight = times(op_far, before + far_folds[p, level, c])
                tops[p, level + 1, c] = before - weight

                @pl.when(level + 1 < steps)
                def _():
                    top_copy(p, level + 1, c, stride * 2).start()

                @pl.when((level + 1 == steps) & not_root)
                def _():
                    fold(p, c)

            each_chunk(upper)
            if p == 0:
                for hop in range(2, half + 1):

                    @pl.when(level == hop - 2)
                    def _():
                        with jax.named_scope("relay"):
                            relay(1, hop)

            return stride * 2

        lax.fori_loop(0, steps, level_step, jnp.int32(1))

        @pl.when(not_root)
        def _():
            for pair in range(pairs):
                both = chunks_of(pair)
                with jax.named_scope("wait_top"):
                    for c in both:
                        top_copy(p, 0, c, 0).wait_recv()
                gained = [far_tops[p, c] + folds[p, c] for c in both]
                weight = times(op_g, jnp.concatenate(gained, axis=1))
                lost = times(op_u, weight)
                before = [tops[p, steps, c] for c in both]
                x[pl.ds(0, width), pl.ds(pair * PAIR, PAIR)] = (
                    jnp.concatenate(before, axis=1) - lost
                )

        @pl.when(d == 0)
        def _():
            for c in range(chunks):
                x[block, pl.ds(c * LANES, LANES)] = tops[p, levels, c]

        if p == 0:
            for hop in range(2, half + 1):

                @pl.when(steps <= hop - 2)
                def _():
                    with jax.named_scope("relay"):
                        relay(1, hop)

    for copy in loads[:4]:
        copy.wait()
    for hop in range(1, half + 1):
        with jax.named_scope("ring"):
            relay(0, hop)
    for copy in loads[4:]:
        copy.wait()
    relay(1, 1)
    panel(0, jnp.int32(0))
    panel(1, jnp.where(d == 0, width, 0))

    for p in range(2):
        for piece in range(4):
            for way in range(2):
                for hop in range(1, hops(piece, way) + 1):
                    ring_copy(p, piece, way, hop, True).wait_send()

        def sent_tops(level, carry):
            each_chunk(lambda c: top_copy(p, level, c, 0).wait_send())
            return carry

        lax.fori_loop(0, steps, sent_tops, 0)

        @pl.when(not_root)
        def _():
            mixer_copy(p, steps).wait_send()
            each_chunk(lambda c: fold_copy(p, c, steps).wait_send())


def local(levels, ring_size, matrix, *reflectors):
    rows, cols = matrix.shape
    turned = [r.T for r in reflectors]
    width = turned[1].shape[1]
    chunks = cols // LANES
    half = ring_size // 2
    vmem, dma = pltpu.VMEM, pltpu.SemaphoreType.DMA
    anywhere = pl.BlockSpec(memory_space=pltpu.HBM)
    tile = (chunks, width, LANES)
    flops = 2 * 3 * 2 * cols * width * (3 * rows + 9 * width)
    arrays = (matrix, *turned)
    return pl.pallas_call(
        functools.partial(kernel, levels, ring_size),
        out_shape=jax.ShapeDtypeStruct(matrix.shape, matrix.dtype),
        in_specs=[anywhere] * 9,
        out_specs=pl.BlockSpec(memory_space=pltpu.VMEM),
        scratch_shapes=[
            vmem((2, width, rows + width), F32),
            vmem((2, width, 2 * width), F32),
            vmem((2, levels, width, width), F32),
            vmem((2, levels + 1, *tile), F32),
            vmem((2, levels, *tile), F32),
            vmem((2, *tile), F32),
            vmem((2, *tile), F32),
            vmem((rows, 3 * width), BF16),
            vmem((width, 3 * rows), BF16),
            vmem((width, 3 * width), BF16),
            vmem((width, 3 * width), BF16),
            vmem((width, 3 * width), BF16),
            vmem((width, 3 * width), BF16),
            vmem((width, 3 * width), BF16),
            dma((2, 4)),
            dma(()),
            dma((2, 4, 2, half)),
            dma((2, 4, 2, half)),
            dma((2, chunks)),
            dma((2, levels, chunks)),
            dma((2, levels, chunks)),
            dma((2, chunks)),
            dma((2,)),
            dma((2, levels)),
        ],
        compiler_params=pltpu.CompilerParams(
            collective_id=0, has_side_effects=True, vmem_limit_bytes=50_331_648
        ),
        cost_estimate=pl.CostEstimate(
            flops=flops, bytes_accessed=8 * rows * cols, transcendentals=0
        ),
        name="tree_update",
    )(*(pltpu.with_memory_space_constraint(a, pltpu.HBM) for a in arrays))


def solution(mesh):
    levels = mesh.shape["row"].bit_length() - 1
    placed = P("row", "col")
    return jax.shard_map(
        functools.partial(local, levels, mesh.shape["col"]),
        mesh=mesh,
        in_specs=(placed,) * 9,
        out_specs=placed,
        check_vma=False,
    )
```

```python
import functools

import jax
import jax.numpy as jnp
from jax import lax
from jax.experimental import pallas as pl
from jax.experimental.pallas import tpu as pltpu
from jax.sharding import PartitionSpec as P

LANES = 128
PAIR = 256
MESH = pl.DeviceIdType.MESH
F32 = jnp.float32
BF16 = jnp.bfloat16


def halves(value):
    high = value.astype(BF16)
    return high, (value - high.astype(F32)).astype(BF16)


def left_operand(value):
    high, low = halves(value)
    return jnp.concatenate([high, high, low], axis=1)


def times(operator, value):
    high, low = halves(value)
    right = jnp.concatenate([high, low, high], axis=0)
    return jnp.dot(operator[...], right, preferred_element_type=F32)


def lower_triangle(value):
    row = lax.broadcasted_iota(jnp.int32, value.shape, 0)
    col = lax.broadcasted_iota(jnp.int32, value.shape, 1)
    return jnp.where(col <= row, value, 0.0)


def kernel(
    levels,
    ring_size,
    matrix,
    v1,
    f1,
    u1,
    g1,
    v2,
    f2,
    u2,
    g2,
    x,
    leafs,
    trees,
    far_mixers,
    tops,
    far_folds,
    folds,
    far_tops,
    op_v,
    op_vt,
    op_f,
    op_u,
    op_ut,
    op_g,
    op_far,
    load_sem,
    x_sem,
    ring_send,
    ring_recv,
    fold_send,
    fold_recv,
    top_send,
    top_recv,
    mixer_send,
    mixer_recv,
):
    rows, columns = x.shape
    chunks = columns // LANES
    pairs = columns // PAIR
    width = trees.shape[1]
    share = width // ring_size
    half = ring_size // 2

    d = lax.axis_index("row")
    k = lax.axis_index("col")
    right = lax.rem(k + 1, ring_size)
    left = lax.rem(k + ring_size - 1, ring_size)
    steps = jnp.int32(0)
    reach = jnp.int32(1)
    for i in range(levels):
        one = jnp.where(lax.rem(d, 2 ** (i + 1)) == 0, 1, 0)
        steps = steps + one
        reach = reach + one * 2**i
    not_root = d != 0
    parent = d - reach

    own = pl.ds(pl.multiple_of(k * share, share), share)
    loads = []
    for p, (v, f, u, g) in enumerate(((v1, f1, u1, g1), (v2, f2, u2, g2))):
        places = (
            (v, leafs.at[p, own, pl.ds(0, rows)]),
            (f, leafs.at[p, own, pl.ds(rows, width)]),
            (u, trees.at[p, own, pl.ds(0, width)]),
            (g, trees.at[p, own, pl.ds(width, width)]),
        )
        for i, (source, place) in enumerate(places):
            loads.append(pltpu.make_async_copy(source, place, load_sem.at[p, i]))
    x_load = pltpu.make_async_copy(matrix, x, x_sem)

    barrier = pltpu.get_barrier_semaphore()

    def greet(row, col):
        pl.semaphore_signal(barrier, inc=1, device_id=(row, col), device_id_type=MESH)

    greet(d, left)
    greet(d, right)

    def greet_lower(i, stride):
        greet(d + stride, k)
        return stride * 2

    lax.fori_loop(0, steps, greet_lower, jnp.int32(1))

    @pl.when(not_root)
    def _():
        greet(parent, k)

    for copy in loads[:4] + [x_load] + loads[4:]:
        copy.start()
    with jax.named_scope("barrier"):
        pl.semaphore_wait(barrier, 2 + steps + jnp.where(not_root, 1, 0))

    starts = ((0, 2 * LANES), (2 * LANES, rows - LANES), (0, width), (width, width))

    def hops(piece, way):
        return half if piece % 2 == way else half - 1

    def ring_copy(p, piece, way, hop, sent):
        back = hop - 1 if sent else hop
        shard = lax.rem(k + (ring_size - back if way == 0 else back), ring_size)
        row = pl.ds(pl.multiple_of(shard * share, share), share)
        start, size = starts[piece]
        if piece < 2:
            first = ((shard * share) // LANES) * LANES
            lanes = pl.ds(pl.multiple_of(first + start, LANES), size)
            ref = leafs.at[p, row, lanes]
        else:
            ref = trees.at[p, row, pl.ds(start, size)]
        return pltpu.make_async_remote_copy(
            src_ref=ref,
            dst_ref=ref,
            send_sem=ring_send.at[p, piece, way, hop - 1],
            recv_sem=ring_recv.at[p, piece, way, hop - 1],
            device_id=(d, right if way == 0 else left),
            device_id_type=MESH,
        )

    def relay(p, hop):
        for piece in range(4):
            for way in range(2):
                if hop <= hops(piece, way):
                    if hop > 1:
                        ring_copy(p, piece, way, hop - 1, False).wait_recv()
                    ring_copy(p, piece, way, hop, True).start()

    def gathered(p, pieces):
        for piece in pieces:
            for way in range(2):
                if hops(piece, way) > 0:
                    ring_copy(p, piece, way, hops(piece, way), False).wait_recv()

    def top_copy(p, level, c, stride):
        return pltpu.make_async_remote_copy(
            src_ref=tops.at[p, level, c],
            dst_ref=far_tops.at[p, c],
            send_sem=top_send.at[p, level, c],
            recv_sem=top_recv.at[p, c],
            device_id=(d + stride, k),
            device_id_type=MESH,
        )

    def fold_copy(p, c, level):
        return pltpu.make_async_remote_copy(
            src_ref=folds.at[p, c],
            dst_ref=far_folds.at[p, level, c],
            send_sem=fold_send.at[p, c],
            recv_sem=fold_recv.at[p, level, c],
            device_id=(parent, k),
            device_id_type=MESH,
        )

    def mixer_copy(p, level):
        return pltpu.make_async_remote_copy(
            src_ref=trees.at[p, :, pl.ds(width, width)],
            dst_ref=far_mixers.at[p, level],
            send_sem=mixer_send.at[p],
            recv_sem=mixer_recv.at[p, level],
            device_id=(parent, k),
            device_id_type=MESH,
        )

    def fold(p, c):
        folds[p, c] = times(op_ut, tops[p, steps, c])
        fold_copy(p, c, steps).start()

    def chunks_of(pair):
        return range(pair * (PAIR // LANES), (pair + 1) * (PAIR // LANES))

    def each_chunk(body):
        def step(c, carry):
            body(c)
            return carry

        lax.fori_loop(0, chunks, step, 0)

    def prepare_leaf(p, offset):
        raw = leafs[p, :, pl.ds(0, rows)]
        row = lax.broadcasted_iota(jnp.int32, raw.shape, 1) - offset
        col = lax.broadcasted_iota(jnp.int32, raw.shape, 0)
        vectors = jnp.where(row > col, raw, jnp.where(row == col, 1.0, 0.0))
        op_vt[...] = left_operand(vectors)
        op_v[...] = left_operand(vectors.T)
        op_f[...] = left_operand(lower_triangle(leafs[p, :, pl.ds(rows, width)]))

    def prepare_tree(p):
        merge = lower_triangle(trees[p, :, pl.ds(0, width)])
        op_ut[...] = left_operand(merge)
        op_u[...] = left_operand(merge.T)
        op_g[...] = left_operand(lower_triangle(trees[p, :, pl.ds(width, width)]))

    def panel(p, offset):
        block = pl.ds(pl.multiple_of(offset, width), width)
        with jax.named_scope("wait_vectors"):
            gathered(p, (0, 1))
        with jax.named_scope("prepare_leaf"):
            prepare_leaf(p, offset)
        if p == 0:
            x_load.wait()

        with jax.named_scope("leaf"):
            for pair in range(pairs):
                lanes = pl.ds(pair * PAIR, PAIR)
                before = x[:, lanes]
                mixed = times(op_f, times(op_vt, before))
                x[:, lanes] = before - times(op_v, mixed)
                for c in chunks_of(pair):
                    tops[p, 0, c] = x[block, pl.ds(c * LANES, LANES)]

                    @pl.when(steps > 0)
                    def _():
                        top_copy(p, 0, c, 1).start()
        with jax.named_scope("wait_merges"):
            gathered(p, (2, 3))

        @pl.when(not_root)
        def _():
            mixer_copy(p, steps).start()

        with jax.named_scope("prepare_tree"):
            prepare_tree(p)

        @pl.when(steps == 0)
        def _():
            with jax.named_scope("first_fold"):
                each_chunk(functools.partial(fold, p))

        def level_step(level, stride):
            prepare_far(p, level, 0)
            each_chunk(functools.partial(upper, p, level, stride, 0))
            if p == 0:
                for hop in range(2, half + 1):

                    @pl.when(level == hop - 2)
                    def _():
                        with jax.named_scope("relay"):
                            relay(1, hop)

            return stride * 2

        near = max(levels - 3, 0)
        lax.fori_loop(0, jnp.minimum(steps, near), level_step, jnp.int32(1))

        @pl.when(steps > near)
        def _():
            prepare_far(p, near, 0)

            @pl.when(steps > near + 1)
            def _():
                prepare_far(p, near + 1, 1)

            def two_levels(c):
                upper(p, near, 2**near, 0, c)

                @pl.when(steps > near + 1)
                def _():
                    upper(p, near + 1, 2 ** (near + 1), 1, c)

            each_chunk(two_levels)

    def prepare_far(p, level, slot):
        with jax.named_scope("wait_mixer"):
            mixer_copy(p, level).wait_recv()
        op_far[slot] = left_operand(lower_triangle(far_mixers[p, level]))

    def upper(p, level, stride, slot, c):
        with jax.named_scope("wait_fold"):
            fold_copy(p, c, level).wait_recv()
        before = tops[p, level, c]
        weight = times(op_far.at[slot], before + far_folds[p, level, c])
        tops[p, level + 1, c] = before - weight

        @pl.when(level + 1 < steps)
        def _():
            top_copy(p, level + 1, c, stride * 2).start()

        @pl.when((level + 1 == steps) & not_root)
        def _():
            fold(p, c)

    def lower(p):
        for pair in range(pairs):
            both = chunks_of(pair)
            with jax.named_scope("wait_top"):
                for c in both:
                    top_copy(p, 0, c, 0).wait_recv()
            gained = [far_tops[p, c] + folds[p, c] for c in both]
            weight = times(op_g, jnp.concatenate(gained, axis=1))
            lost = times(op_u, weight)
            before = [tops[p, steps, c] for c in both]
            x[pl.ds(0, width), pl.ds(pair * PAIR, PAIR)] = (
                jnp.concatenate(before, axis=1) - lost
            )

    def root(p, first):
        last = levels - 1
        prepare_far(p, last, 0)
        for c in range(chunks):
            upper(p, last, 2**last, 0, c)
            x[pl.ds(first, width), pl.ds(c * LANES, LANES)] = tops[p, levels, c]

    for copy in loads[:4]:
        copy.wait()
    for hop in range(1, half + 1):
        with jax.named_scope("ring"):
            relay(0, hop)
    for copy in loads[4:]:
        copy.wait()
    relay(1, 1)
    panel(0, jnp.int32(0))

    @pl.when(not_root)
    def _():
        lower(0)

    for hop in range(2, half + 1):

        @pl.when(jnp.minimum(steps, max(levels - 3, 0)) <= hop - 2)
        def _():
            with jax.named_scope("relay"):
                relay(1, hop)

    panel(1, jnp.where(not_root, 0, width))

    @pl.when(not_root)
    def _():
        lower(1)

    @pl.when(d == 0)
    def _():
        root(0, 0)
        root(1, width)

    for p in range(2):
        for piece in range(4):
            for way in range(2):
                for hop in range(1, hops(piece, way) + 1):
                    ring_copy(p, piece, way, hop, True).wait_send()

        def sent_tops(level, carry):
            each_chunk(lambda c: top_copy(p, level, c, 0).wait_send())
            return carry

        lax.fori_loop(0, steps, sent_tops, 0)

        @pl.when(not_root)
        def _():
            mixer_copy(p, steps).wait_send()
            each_chunk(lambda c: fold_copy(p, c, steps).wait_send())


def local(levels, ring_size, matrix, *reflectors):
    rows, cols = matrix.shape
    turned = [r.T for r in reflectors]
    width = turned[1].shape[1]
    chunks = cols // LANES
    half = ring_size // 2
    vmem, dma = pltpu.VMEM, pltpu.SemaphoreType.DMA
    anywhere = pl.BlockSpec(memory_space=pltpu.HBM)
    tile = (chunks, width, LANES)
    flops = 2 * 3 * 2 * cols * width * (3 * rows + 9 * width)
    arrays = (matrix, *turned)
    return pl.pallas_call(
        functools.partial(kernel, levels, ring_size),
        out_shape=jax.ShapeDtypeStruct(matrix.shape, matrix.dtype),
        in_specs=[anywhere] * 9,
        out_specs=pl.BlockSpec(memory_space=pltpu.VMEM),
        scratch_shapes=[
            vmem((2, width, rows + width), F32),
            vmem((2, width, 2 * width), F32),
            vmem((2, levels, width, width), F32),
            vmem((2, levels + 1, *tile), F32),
            vmem((2, levels, *tile), F32),
            vmem((2, *tile), F32),
            vmem((2, *tile), F32),
            vmem((rows, 3 * width), BF16),
            vmem((width, 3 * rows), BF16),
            vmem((width, 3 * width), BF16),
            vmem((width, 3 * width), BF16),
            vmem((width, 3 * width), BF16),
            vmem((width, 3 * width), BF16),
            vmem((2, width, 3 * width), BF16),
            dma((2, 4)),
            dma(()),
            dma((2, 4, 2, half)),
            dma((2, 4, 2, half)),
            dma((2, chunks)),
            dma((2, levels, chunks)),
            dma((2, levels, chunks)),
            dma((2, chunks)),
            dma((2,)),
            dma((2, levels)),
        ],
        compiler_params=pltpu.CompilerParams(
            collective_id=0, has_side_effects=True, vmem_limit_bytes=50_331_648
        ),
        cost_estimate=pl.CostEstimate(
            flops=flops, bytes_accessed=8 * rows * cols, transcendentals=0
        ),
        name="tree_update",
    )(*(pltpu.with_memory_space_constraint(a, pltpu.HBM) for a in arrays))


def solution(mesh):
    levels = mesh.shape["row"].bit_length() - 1
    placed = P("row", "col")
    return jax.shard_map(
        functools.partial(local, levels, mesh.shape["col"]),
        mesh=mesh,
        in_specs=(placed,) * 9,
        out_specs=placed,
        check_vma=False,
    )
```

```python
import functools

import jax
import jax.numpy as jnp
from jax import lax
from jax.experimental import pallas as pl
from jax.experimental.pallas import tpu as pltpu
from jax.sharding import PartitionSpec as P

LANES = 128
PAIR = 256
CHAINED = (2, 4, 5)
MESH = pl.DeviceIdType.MESH
F32 = jnp.float32
BF16 = jnp.bfloat16


def halves(value):
    high = value.astype(BF16)
    return high, (value - high.astype(F32)).astype(BF16)


def left_operand(value):
    high, low = halves(value)
    return jnp.concatenate([high, high, low], axis=1)


def times(operator, value):
    high, low = halves(value)
    right = jnp.concatenate([high, low, high], axis=0)
    return jnp.dot(operator[...], right, preferred_element_type=F32)


def lower_triangle(value):
    row = lax.broadcasted_iota(jnp.int32, value.shape, 0)
    col = lax.broadcasted_iota(jnp.int32, value.shape, 1)
    return jnp.where(col <= row, value, 0.0)


def kernel(
    levels,
    ring_size,
    matrix,
    v1,
    f1,
    u1,
    g1,
    v2,
    f2,
    u2,
    g2,
    x,
    leafs,
    trees,
    far_mixers,
    tops,
    far_folds,
    folds,
    far_tops,
    passed,
    op_v,
    op_vt,
    op_f,
    op_u,
    op_ut,
    op_g,
    op_far,
    load_sem,
    x_sem,
    ring_send,
    ring_recv,
    fold_send,
    fold_recv,
    top_send,
    top_recv,
    pass_send,
    mixer_send,
    mixer_recv,
):
    rows, columns = x.shape
    chunks = columns // LANES
    pairs = columns // PAIR
    width = trees.shape[1]
    share = width // ring_size
    half = ring_size // 2

    d = lax.axis_index("row")
    k = lax.axis_index("col")
    right = lax.rem(k + 1, ring_size)
    left = lax.rem(k + ring_size - 1, ring_size)
    steps = jnp.int32(0)
    reach = jnp.int32(1)
    for i in range(levels):
        one = jnp.where(lax.rem(d, 2 ** (i + 1)) == 0, 1, 0)
        steps = steps + one
        reach = reach + one * 2**i
    not_root = d != 0
    parent = d - reach
    hands_on = jnp.int32(0)
    handed = jnp.int32(0)
    for i in CHAINED:
        if i < levels:
            hands_on = hands_on + jnp.where(lax.rem(d, 2 ** (i + 1)) == 2 ** (i - 1), 1, 0)
            handed = handed + jnp.where(lax.rem(d, 2 ** (i + 1)) == 2**i, 1, 0)
    before_me = d - reach // 2
    after_me = d + reach

    own = pl.ds(pl.multiple_of(k * share, share), share)
    loads = []
    for p, (v, f, u, g) in enumerate(((v1, f1, u1, g1), (v2, f2, u2, g2))):
        places = (
            (v, leafs.at[p, own, pl.ds(0, rows)]),
            (f, leafs.at[p, own, pl.ds(rows, width)]),
            (u, trees.at[p, own, pl.ds(0, width)]),
            (g, trees.at[p, own, pl.ds(width, width)]),
        )
        for i, (source, place) in enumerate(places):
            loads.append(pltpu.make_async_copy(source, place, load_sem.at[p, i]))
    x_load = pltpu.make_async_copy(matrix, x, x_sem)

    barrier = pltpu.get_barrier_semaphore()

    def greet(row, col):
        pl.semaphore_signal(barrier, inc=1, device_id=(row, col), device_id_type=MESH)

    greet(d, left)
    greet(d, right)

    def greet_lower(i, stride):
        greet(d + stride, k)
        return stride * 2

    lax.fori_loop(0, steps, greet_lower, jnp.int32(1))

    @pl.when(not_root)
    def _():
        greet(parent, k)

    @pl.when(hands_on > 0)
    def _():
        greet(after_me, k)

    @pl.when(handed > 0)
    def _():
        greet(before_me, k)

    for copy in loads[:4] + [x_load] + loads[4:]:
        copy.start()
    with jax.named_scope("barrier"):
        pl.semaphore_wait(
            barrier, 2 + steps + jnp.where(not_root, 1, 0) + hands_on + handed
        )

    starts = ((0, 2 * LANES), (2 * LANES, rows - LANES), (0, width), (width, width))

    def hops(piece, way):
        return half if piece % 2 == way else half - 1

    def ring_copy(p, piece, way, hop, sent):
        back = hop - 1 if sent else hop
        shard = lax.rem(k + (ring_size - back if way == 0 else back), ring_size)
        row = pl.ds(pl.multiple_of(shard * share, share), share)
        start, size = starts[piece]
        if piece < 2:
            first = ((shard * share) // LANES) * LANES
            lanes = pl.ds(pl.multiple_of(first + start, LANES), size)
            ref = leafs.at[p, row, lanes]
        else:
            ref = trees.at[p, row, pl.ds(start, size)]
        return pltpu.make_async_remote_copy(
            src_ref=ref,
            dst_ref=ref,
            send_sem=ring_send.at[p, piece, way, hop - 1],
            recv_sem=ring_recv.at[p, piece, way, hop - 1],
            device_id=(d, right if way == 0 else left),
            device_id_type=MESH,
        )

    def relay(p, hop):
        for piece in range(4):
            for way in range(2):
                if hop <= hops(piece, way):
                    if hop > 1:
                        ring_copy(p, piece, way, hop - 1, False).wait_recv()
                    ring_copy(p, piece, way, hop, True).start()

    def gathered(p, pieces):
        for piece in pieces:
            for way in range(2):
                if hops(piece, way) > 0:
                    ring_copy(p, piece, way, hops(piece, way), False).wait_recv()

    def top_copy(p, level, c, stride):
        return pltpu.make_async_remote_copy(
            src_ref=tops.at[p, level, c],
            dst_ref=far_tops.at[p, c],
            send_sem=top_send.at[p, level, c],
            recv_sem=top_recv.at[p, c],
            device_id=(d + stride, k),
            device_id_type=MESH,
        )

    def pass_copy(p, c):
        return pltpu.make_async_remote_copy(
            src_ref=passed.at[p, c],
            dst_ref=far_tops.at[p, c],
            send_sem=pass_send.at[p, c],
            recv_sem=top_recv.at[p, c],
            device_id=(after_me, k),
            device_id_type=MESH,
        )

    def sends_top(level):
        sends = level < steps
        for i in CHAINED:
            sends = sends & (level != i)
        return sends

    def fold_copy(p, c, level):
        return pltpu.make_async_remote_copy(
            src_ref=folds.at[p, c],
            dst_ref=far_folds.at[p, level, c],
            send_sem=fold_send.at[p, c],
            recv_sem=fold_recv.at[p, level, c],
            device_id=(parent, k),
            device_id_type=MESH,
        )

    def mixer_copy(p, level):
        return pltpu.make_async_remote_copy(
            src_ref=trees.at[p, :, pl.ds(width, width)],
            dst_ref=far_mixers.at[p, level],
            send_sem=mixer_send.at[p],
            recv_sem=mixer_recv.at[p, level],
            device_id=(parent, k),
            device_id_type=MESH,
        )

    def fold(p, c):
        folds[p, c] = times(op_ut, tops[p, steps, c])
        fold_copy(p, c, steps).start()

    def chunks_of(pair):
        return range(pair * (PAIR // LANES), (pair + 1) * (PAIR // LANES))

    def each_chunk(body):
        def step(c, carry):
            body(c)
            return carry

        lax.fori_loop(0, chunks, step, 0)

    def prepare_leaf(p, offset):
        raw = leafs[p, :, pl.ds(0, rows)]
        row = lax.broadcasted_iota(jnp.int32, raw.shape, 1) - offset
        col = lax.broadcasted_iota(jnp.int32, raw.shape, 0)
        vectors = jnp.where(row > col, raw, jnp.where(row == col, 1.0, 0.0))
        op_vt[...] = left_operand(vectors)
        op_v[...] = left_operand(vectors.T)
        op_f[...] = left_operand(lower_triangle(leafs[p, :, pl.ds(rows, width)]))

    def prepare_tree(p):
        merge = lower_triangle(trees[p, :, pl.ds(0, width)])
        op_ut[...] = left_operand(merge)
        op_u[...] = left_operand(merge.T)
        op_g[...] = left_operand(lower_triangle(trees[p, :, pl.ds(width, width)]))

    def panel(p, offset):
        block = pl.ds(pl.multiple_of(offset, width), width)
        with jax.named_scope("wait_vectors"):
            gathered(p, (0, 1))
        with jax.named_scope("prepare_leaf"):
            prepare_leaf(p, offset)
        if p == 0:
            x_load.wait()

        with jax.named_scope("leaf"):
            for pair in range(pairs):
                lanes = pl.ds(pair * PAIR, PAIR)
                before = x[:, lanes]
                mixed = times(op_f, times(op_vt, before))
                x[:, lanes] = before - times(op_v, mixed)
                for c in chunks_of(pair):
                    tops[p, 0, c] = x[block, pl.ds(c * LANES, LANES)]

                    @pl.when(steps > 0)
                    def _():
                        top_copy(p, 0, c, 1).start()
        with jax.named_scope("wait_merges"):
            gathered(p, (2, 3))

        @pl.when(not_root)
        def _():
            mixer_copy(p, steps).start()

        with jax.named_scope("prepare_tree"):
            prepare_tree(p)

        @pl.when(steps == 0)
        def _():
            with jax.named_scope("first_fold"):
                each_chunk(functools.partial(fold, p))

        def level_step(level, stride):
            prepare_far(p, level, 0)
            each_chunk(functools.partial(upper, p, level, stride, 0))
            if p == 0:
                for hop in range(3, half + 1):

                    @pl.when(level == hop - 2)
                    def _():
                        with jax.named_scope("relay"):
                            relay(1, hop)

            return stride * 2

        if p == 0 and half > 1:
            with jax.named_scope("relay"):
                relay(1, 2)

        near = max(levels - 3, 0)
        lax.fori_loop(0, jnp.minimum(steps, near), level_step, jnp.int32(1))

        @pl.when(steps > near)
        def _():
            prepare_far(p, near, 0)

            @pl.when(steps > near + 1)
            def _():
                prepare_far(p, near + 1, 1)

            def two_levels(c):
                upper(p, near, 2**near, 0, c)

                @pl.when(steps > near + 1)
                def _():
                    upper(p, near + 1, 2 ** (near + 1), 1, c)

            each_chunk(two_levels)

    def prepare_far(p, level, slot):
        with jax.named_scope("wait_mixer"):
            mixer_copy(p, level).wait_recv()
        op_far[slot] = left_operand(lower_triangle(far_mixers[p, level]))

    def upper(p, level, stride, slot, c):
        with jax.named_scope("wait_fold"):
            fold_copy(p, c, level).wait_recv()
        before = tops[p, level, c]
        weight = times(op_far.at[slot], before + far_folds[p, level, c])
        tops[p, level + 1, c] = before - weight

        @pl.when(sends_top(level + 1))
        def _():
            top_copy(p, level + 1, c, stride * 2).start()

        @pl.when((level + 1 == steps) & not_root)
        def _():
            fold(p, c)

    def lower(p):
        for c in range(chunks):
            with jax.named_scope("wait_top"):
                top_copy(p, 0, c, 0).wait_recv()
            upper_rows = far_tops[p, c]
            weight = times(op_g, upper_rows + folds[p, c])

            @pl.when(hands_on > 0)
            def _():
                passed[p, c] = upper_rows - weight
                pass_copy(p, c).start()

            x[pl.ds(0, width), pl.ds(c * LANES, LANES)] = (
                tops[p, steps, c] - times(op_u, weight)
            )

    def root(p, first):
        last = levels - 1
        prepare_far(p, last, 0)
        for c in range(chunks):
            upper(p, last, 2**last, 0, c)
            x[pl.ds(first, width), pl.ds(c * LANES, LANES)] = tops[p, levels, c]

    for copy in loads[:4]:
        copy.wait()
    for hop in range(1, half + 1):
        with jax.named_scope("ring"):
            relay(0, hop)
    for copy in loads[4:]:
        copy.wait()
    relay(1, 1)
    panel(0, jnp.int32(0))

    @pl.when(not_root)
    def _():
        lower(0)

    for hop in range(3, half + 1):

        @pl.when(jnp.minimum(steps, max(levels - 3, 0)) <= hop - 2)
        def _():
            with jax.named_scope("relay"):
                relay(1, hop)

    panel(1, jnp.where(not_root, 0, width))

    @pl.when(not_root)
    def _():
        lower(1)

    @pl.when(d == 0)
    def _():
        root(0, 0)
        root(1, width)

    for p in range(2):
        for piece in range(4):
            for way in range(2):
                for hop in range(1, hops(piece, way) + 1):
                    ring_copy(p, piece, way, hop, True).wait_send()

        def sent_tops(level, carry):
            @pl.when(sends_top(level))
            def _():
                each_chunk(lambda c: top_copy(p, level, c, 0).wait_send())

            return carry

        lax.fori_loop(0, steps, sent_tops, 0)

        @pl.when(hands_on > 0)
        def _():
            each_chunk(lambda c: pass_copy(p, c).wait_send())

        @pl.when(not_root)
        def _():
            mixer_copy(p, steps).wait_send()
            each_chunk(lambda c: fold_copy(p, c, steps).wait_send())


def local(levels, ring_size, matrix, *reflectors):
    rows, cols = matrix.shape
    turned = [r.T for r in reflectors]
    width = turned[1].shape[1]
    chunks = cols // LANES
    half = ring_size // 2
    vmem, dma = pltpu.VMEM, pltpu.SemaphoreType.DMA
    anywhere = pl.BlockSpec(memory_space=pltpu.HBM)
    tile = (chunks, width, LANES)
    flops = 2 * 3 * 2 * cols * width * (3 * rows + 9 * width)
    arrays = (matrix, *turned)
    return pl.pallas_call(
        functools.partial(kernel, levels, ring_size),
        out_shape=jax.ShapeDtypeStruct(matrix.shape, matrix.dtype),
        in_specs=[anywhere] * 9,
        out_specs=pl.BlockSpec(memory_space=pltpu.VMEM),
        scratch_shapes=[
            vmem((2, width, rows + width), F32),
            vmem((2, width, 2 * width), F32),
            vmem((2, levels, width, width), F32),
            vmem((2, levels + 1, *tile), F32),
            vmem((2, levels, *tile), F32),
            vmem((2, *tile), F32),
            vmem((2, *tile), F32),
            vmem((2, *tile), F32),
            vmem((rows, 3 * width), BF16),
            vmem((width, 3 * rows), BF16),
            vmem((width, 3 * width), BF16),
            vmem((width, 3 * width), BF16),
            vmem((width, 3 * width), BF16),
            vmem((width, 3 * width), BF16),
            vmem((2, width, 3 * width), BF16),
            dma((2, 4)),
            dma(()),
            dma((2, 4, 2, half)),
            dma((2, 4, 2, half)),
            dma((2, chunks)),
            dma((2, levels, chunks)),
            dma((2, levels, chunks)),
            dma((2, chunks)),
            dma((2, chunks)),
            dma((2,)),
            dma((2, levels)),
        ],
        compiler_params=pltpu.CompilerParams(
            collective_id=0, has_side_effects=True, vmem_limit_bytes=50_331_648
        ),
        cost_estimate=pl.CostEstimate(
            flops=flops, bytes_accessed=8 * rows * cols, transcendentals=0
        ),
        name="tree_update",
    )(*(pltpu.with_memory_space_constraint(a, pltpu.HBM) for a in arrays))


def solution(mesh):
    levels = mesh.shape["row"].bit_length() - 1
    placed = P("row", "col")
    return jax.shard_map(
        functools.partial(local, levels, mesh.shape["col"]),
        mesh=mesh,
        in_specs=(placed,) * 9,
        out_specs=placed,
        check_vma=False,
    )
```

```python
import functools

import jax
import jax.numpy as jnp
from jax import lax
from jax.experimental import pallas as pl
from jax.experimental.pallas import tpu as pltpu
from jax.sharding import PartitionSpec as P

LANES = 128
PAIR = 256
CHAINED = (2, 4, 5)
MESH = pl.DeviceIdType.MESH
F32 = jnp.float32
BF16 = jnp.bfloat16


def halves(value):
    high = value.astype(BF16)
    return high, (value - high.astype(F32)).astype(BF16)


def left_operand(value):
    high, low = halves(value)
    return jnp.concatenate([high, high, low], axis=1)


def times(operator, value):
    high, low = halves(value)
    right = jnp.concatenate([high, low, high], axis=0)
    return jnp.dot(operator[...], right, preferred_element_type=F32)


def lower_triangle(value):
    row = lax.broadcasted_iota(jnp.int32, value.shape, 0)
    col = lax.broadcasted_iota(jnp.int32, value.shape, 1)
    return jnp.where(col <= row, value, 0.0)


def kernel(
    levels,
    ring_size,
    matrix,
    v1,
    f1,
    u1,
    g1,
    v2,
    f2,
    u2,
    g2,
    x,
    leafs,
    trees,
    far_mixers,
    tops,
    far_folds,
    folds,
    far_tops,
    passed,
    op_v,
    op_vt,
    op_f,
    op_u,
    op_ut,
    op_g,
    op_far,
    load_sem,
    x_sem,
    ring_send,
    ring_recv,
    fold_send,
    fold_recv,
    top_send,
    top_recv,
    pass_send,
    mixer_send,
    mixer_recv,
):
    rows, columns = x.shape
    chunks = columns // LANES
    pairs = columns // PAIR
    width = trees.shape[1]
    share = width // ring_size
    half = ring_size // 2

    d = lax.axis_index("row")
    k = lax.axis_index("col")
    right = lax.rem(k + 1, ring_size)
    left = lax.rem(k + ring_size - 1, ring_size)
    steps = jnp.int32(0)
    reach = jnp.int32(1)
    for i in range(levels):
        one = jnp.where(lax.rem(d, 2 ** (i + 1)) == 0, 1, 0)
        steps = steps + one
        reach = reach + one * 2**i
    not_root = d != 0
    parent = d - reach
    hands_on = jnp.int32(0)
    handed = jnp.int32(0)
    for i in CHAINED:
        if i < levels:
            hands_on = hands_on + jnp.where(lax.rem(d, 2 ** (i + 1)) == 2 ** (i - 1), 1, 0)
            handed = handed + jnp.where(lax.rem(d, 2 ** (i + 1)) == 2**i, 1, 0)
    before_me = d - reach // 2
    after_me = d + reach

    own = pl.ds(pl.multiple_of(k * share, share), share)
    loads = []
    for p, (v, f, u, g) in enumerate(((v1, f1, u1, g1), (v2, f2, u2, g2))):
        places = (
            (v, leafs.at[p, own, pl.ds(0, rows)]),
            (f, leafs.at[p, own, pl.ds(rows, width)]),
            (u, trees.at[p, own, pl.ds(0, width)]),
            (g, trees.at[p, own, pl.ds(width, width)]),
        )
        for i, (source, place) in enumerate(places):
            loads.append(pltpu.make_async_copy(source, place, load_sem.at[p, i]))
    x_load = pltpu.make_async_copy(matrix, x, x_sem)

    barrier = pltpu.get_barrier_semaphore()

    def greet(row, col):
        pl.semaphore_signal(barrier, inc=1, device_id=(row, col), device_id_type=MESH)

    greet(d, left)
    greet(d, right)

    def greet_lower(i, stride):
        greet(d + stride, k)
        return stride * 2

    lax.fori_loop(0, steps, greet_lower, jnp.int32(1))

    @pl.when(not_root)
    def _():
        greet(parent, k)

    @pl.when(hands_on > 0)
    def _():
        greet(after_me, k)

    @pl.when(handed > 0)
    def _():
        greet(before_me, k)

    for copy in loads[:4] + [x_load] + loads[4:]:
        copy.start()
    with jax.named_scope("barrier"):
        pl.semaphore_wait(
            barrier, 2 + steps + jnp.where(not_root, 1, 0) + hands_on + handed
        )

    starts = ((0, 2 * LANES), (2 * LANES, rows - LANES), (0, width), (width, width))

    def hops(piece, way):
        return half if piece % 2 == way else half - 1

    def ring_copy(p, piece, way, hop, sent):
        back = hop - 1 if sent else hop
        shard = lax.rem(k + (ring_size - back if way == 0 else back), ring_size)
        row = pl.ds(pl.multiple_of(shard * share, share), share)
        start, size = starts[piece]
        if piece < 2:
            first = ((shard * share) // LANES) * LANES
            lanes = pl.ds(pl.multiple_of(first + start, LANES), size)
            ref = leafs.at[p, row, lanes]
        else:
            ref = trees.at[p, row, pl.ds(start, size)]
        return pltpu.make_async_remote_copy(
            src_ref=ref,
            dst_ref=ref,
            send_sem=ring_send.at[p, piece, way, hop - 1],
            recv_sem=ring_recv.at[p, piece, way, hop - 1],
            device_id=(d, right if way == 0 else left),
            device_id_type=MESH,
        )

    def relay(p, hop):
        for piece in range(4):
            for way in range(2):
                if hop <= hops(piece, way):
                    if hop > 1:
                        ring_copy(p, piece, way, hop - 1, False).wait_recv()
                    ring_copy(p, piece, way, hop, True).start()

    def gathered(p, pieces):
        for piece in pieces:
            for way in range(2):
                if hops(piece, way) > 0:
                    ring_copy(p, piece, way, hops(piece, way), False).wait_recv()

    def top_copy(p, level, c, stride):
        return pltpu.make_async_remote_copy(
            src_ref=tops.at[p, level, c],
            dst_ref=far_tops.at[p, c],
            send_sem=top_send.at[p, level, c],
            recv_sem=top_recv.at[p, c],
            device_id=(d + stride, k),
            device_id_type=MESH,
        )

    def pass_copy(p, c):
        return pltpu.make_async_remote_copy(
            src_ref=passed.at[p, c],
            dst_ref=far_tops.at[p, c],
            send_sem=pass_send.at[p, c],
            recv_sem=top_recv.at[p, c],
            device_id=(after_me, k),
            device_id_type=MESH,
        )

    def sends_top(level):
        sends = level < steps
        for i in CHAINED:
            sends = sends & (level != i)
        return sends

    def fold_copy(p, c, level):
        return pltpu.make_async_remote_copy(
            src_ref=folds.at[p, c],
            dst_ref=far_folds.at[p, level, c],
            send_sem=fold_send.at[p, c],
            recv_sem=fold_recv.at[p, level, c],
            device_id=(parent, k),
            device_id_type=MESH,
        )

    def mixer_copy(p, level):
        return pltpu.make_async_remote_copy(
            src_ref=trees.at[p, :, pl.ds(width, width)],
            dst_ref=far_mixers.at[p, level],
            send_sem=mixer_send.at[p],
            recv_sem=mixer_recv.at[p, level],
            device_id=(parent, k),
            device_id_type=MESH,
        )

    late = steps == levels - 1

    def fold(p, c):
        folds[p, c] = times(op_ut, tops[p, steps, c])

        @pl.when((p > 0) | jnp.logical_not(late))
        def _():
            fold_copy(p, c, steps).start()

    def chunks_of(pair):
        return range(pair * (PAIR // LANES), (pair + 1) * (PAIR // LANES))

    def each_chunk(body):
        def step(c, carry):
            body(c)
            return carry

        lax.fori_loop(0, chunks, step, 0)

    def prepare_leaf(p, offset):
        raw = leafs[p, :, pl.ds(0, rows)]
        row = lax.broadcasted_iota(jnp.int32, raw.shape, 1) - offset
        col = lax.broadcasted_iota(jnp.int32, raw.shape, 0)
        vectors = jnp.where(row > col, raw, jnp.where(row == col, 1.0, 0.0))
        op_vt[...] = left_operand(vectors)
        op_v[...] = left_operand(vectors.T)
        op_f[...] = left_operand(lower_triangle(leafs[p, :, pl.ds(rows, width)]))

    def prepare_tree(p):
        merge = lower_triangle(trees[p, :, pl.ds(0, width)])
        op_ut[...] = left_operand(merge)
        op_u[...] = left_operand(merge.T)
        op_g[...] = left_operand(lower_triangle(trees[p, :, pl.ds(width, width)]))

    def panel(p, offset):
        block = pl.ds(pl.multiple_of(offset, width), width)
        with jax.named_scope("wait_vectors"):
            gathered(p, (0, 1))
        with jax.named_scope("prepare_leaf"):
            prepare_leaf(p, offset)
        if p == 0:
            x_load.wait()

        for pair in range(pairs):
            with jax.named_scope("leaf"):
                lanes = pl.ds(pair * PAIR, PAIR)
                before = x[:, lanes]
                mixed = times(op_f, times(op_vt, before))
                x[:, lanes] = before - times(op_v, mixed)
                for c in chunks_of(pair):
                    tops[p, 0, c] = x[block, pl.ds(c * LANES, LANES)]

                    @pl.when(steps > 0)
                    def _():
                        top_copy(p, 0, c, 1).start()

            if pair == 0:
                with jax.named_scope("wait_merges"):
                    gathered(p, (2, 3))

                @pl.when(not_root)
                def _():
                    mixer_copy(p, steps).start()

        if p == 1:

            @pl.when(late)
            def _():
                each_chunk(lambda c: fold_copy(0, c, steps).start())

        with jax.named_scope("prepare_tree"):
            prepare_tree(p)

        @pl.when(steps == 0)
        def _():
            with jax.named_scope("first_fold"):
                each_chunk(functools.partial(fold, p))

        def level_step(level, stride):
            prepare_far(p, level, 0)
            each_chunk(functools.partial(upper, p, level, stride, 0))
            if p == 0:
                for hop in range(2, half + 1):

                    @pl.when(level == hop - 2)
                    def _():
                        with jax.named_scope("relay"):
                            relay(1, hop)

            return stride * 2

        near = max(levels - 3, 0)
        lax.fori_loop(0, jnp.minimum(steps, near), level_step, jnp.int32(1))

        @pl.when(steps > near)
        def _():
            prepare_far(p, near, 0)

            @pl.when(steps > near + 1)
            def _():
                prepare_far(p, near + 1, 1)

            def two_levels(c):
                upper(p, near, 2**near, 0, c)

                @pl.when(steps > near + 1)
                def _():
                    upper(p, near + 1, 2 ** (near + 1), 1, c)

            each_chunk(two_levels)

    def prepare_far(p, level, slot):
        with jax.named_scope("wait_mixer"):
            mixer_copy(p, level).wait_recv()
        op_far[slot] = left_operand(lower_triangle(far_mixers[p, level]))

    def upper(p, level, stride, slot, c):
        with jax.named_scope("wait_fold"):
            fold_copy(p, c, level).wait_recv()
        before = tops[p, level, c]
        weight = times(op_far.at[slot], before + far_folds[p, level, c])
        tops[p, level + 1, c] = before - weight

        @pl.when(sends_top(level + 1))
        def _():
            top_copy(p, level + 1, c, stride * 2).start()

        @pl.when((level + 1 == steps) & not_root)
        def _():
            fold(p, c)

    def lower(p):
        for c in range(chunks):
            with jax.named_scope("wait_top"):
                top_copy(p, 0, c, 0).wait_recv()
            upper_rows = far_tops[p, c]
            weight = times(op_g, upper_rows + folds[p, c])

            @pl.when(hands_on > 0)
            def _():
                passed[p, c] = upper_rows - weight
                pass_copy(p, c).start()

            x[pl.ds(0, width), pl.ds(c * LANES, LANES)] = (
                tops[p, steps, c] - times(op_u, weight)
            )

    def root(p, first):
        last = levels - 1
        prepare_far(p, last, 0)
        for c in range(chunks):
            upper(p, last, 2**last, 0, c)
            x[pl.ds(first, width), pl.ds(c * LANES, LANES)] = tops[p, levels, c]

    for copy in loads[:4]:
        copy.wait()
    for hop in range(1, half + 1):
        with jax.named_scope("ring"):
            relay(0, hop)
    for copy in loads[4:]:
        copy.wait()
    relay(1, 1)
    panel(0, jnp.int32(0))

    early = (steps == 2) & (levels > 4)
    if half > 3:

        @pl.when(early)
        def _():
            with jax.named_scope("relay"):
                relay(1, 4)

    @pl.when(not_root)
    def _():
        lower(0)

    for hop in range(2, half + 1):
        due = jnp.minimum(steps, max(levels - 3, 0)) <= hop - 2
        if hop == 4:
            due = due & jnp.logical_not(early)

        @pl.when(due)
        def _():
            with jax.named_scope("relay"):
                relay(1, hop)

    panel(1, jnp.where(not_root, 0, width))

    @pl.when(not_root)
    def _():
        lower(1)

    @pl.when(d == 0)
    def _():
        root(0, 0)
        root(1, width)

    for p in range(2):
        for piece in range(4):
            for way in range(2):
                for hop in range(1, hops(piece, way) + 1):
                    ring_copy(p, piece, way, hop, True).wait_send()

        def sent_tops(level, carry):
            @pl.when(sends_top(level))
            def _():
                each_chunk(lambda c: top_copy(p, level, c, 0).wait_send())

            return carry

        lax.fori_loop(0, steps, sent_tops, 0)

        @pl.when(hands_on > 0)
        def _():
            each_chunk(lambda c: pass_copy(p, c).wait_send())

        @pl.when(not_root)
        def _():
            mixer_copy(p, steps).wait_send()
            each_chunk(lambda c: fold_copy(p, c, steps).wait_send())


def local(levels, ring_size, matrix, *reflectors):
    rows, cols = matrix.shape
    turned = [r.T for r in reflectors]
    width = turned[1].shape[1]
    chunks = cols // LANES
    half = ring_size // 2
    vmem, dma = pltpu.VMEM, pltpu.SemaphoreType.DMA
    anywhere = pl.BlockSpec(memory_space=pltpu.HBM)
    tile = (chunks, width, LANES)
    flops = 2 * 3 * 2 * cols * width * (3 * rows + 9 * width)
    arrays = (matrix, *turned)
    return pl.pallas_call(
        functools.partial(kernel, levels, ring_size),
        out_shape=jax.ShapeDtypeStruct(matrix.shape, matrix.dtype),
        in_specs=[anywhere] * 9,
        out_specs=pl.BlockSpec(memory_space=pltpu.VMEM),
        scratch_shapes=[
            vmem((2, width, rows + width), F32),
            vmem((2, width, 2 * width), F32),
            vmem((2, levels, width, width), F32),
            vmem((2, levels + 1, *tile), F32),
            vmem((2, levels, *tile), F32),
            vmem((2, *tile), F32),
            vmem((2, *tile), F32),
            vmem((2, *tile), F32),
            vmem((rows, 3 * width), BF16),
            vmem((width, 3 * rows), BF16),
            vmem((width, 3 * width), BF16),
            vmem((width, 3 * width), BF16),
            vmem((width, 3 * width), BF16),
            vmem((width, 3 * width), BF16),
            vmem((2, width, 3 * width), BF16),
            dma((2, 4)),
            dma(()),
            dma((2, 4, 2, half)),
            dma((2, 4, 2, half)),
            dma((2, chunks)),
            dma((2, levels, chunks)),
            dma((2, levels, chunks)),
            dma((2, chunks)),
            dma((2, chunks)),
            dma((2,)),
            dma((2, levels)),
        ],
        compiler_params=pltpu.CompilerParams(
            collective_id=0, has_side_effects=True, vmem_limit_bytes=50_331_648
        ),
        cost_estimate=pl.CostEstimate(
            flops=flops, bytes_accessed=8 * rows * cols, transcendentals=0
        ),
        name="tree_update",
    )(*(pltpu.with_memory_space_constraint(a, pltpu.HBM) for a in arrays))


def solution(mesh):
    levels = mesh.shape["row"].bit_length() - 1
    placed = P("row", "col")
    return jax.shard_map(
        functools.partial(local, levels, mesh.shape["col"]),
        mesh=mesh,
        in_specs=(placed,) * 9,
        out_specs=placed,
        check_vma=False,
    )
```

```python
import functools

import jax
import jax.numpy as jnp
from jax import lax
from jax.experimental import pallas as pl
from jax.experimental.pallas import tpu as pltpu
from jax.sharding import PartitionSpec as P

LANES = 128
PAIR = 256
CHAINED = (2, 4, 5)
MESH = pl.DeviceIdType.MESH
F32 = jnp.float32
BF16 = jnp.bfloat16


def halves(value):
    high = value.astype(BF16)
    return high, (value - high.astype(F32)).astype(BF16)


def left_operand(value):
    high, low = halves(value)
    return jnp.concatenate([high, high, low], axis=1)


def times(operator, value):
    high, low = halves(value)
    right = jnp.concatenate([high, low, high], axis=0)
    return jnp.dot(operator[...], right, preferred_element_type=F32)


def lower_triangle(value):
    row = lax.broadcasted_iota(jnp.int32, value.shape, 0)
    col = lax.broadcasted_iota(jnp.int32, value.shape, 1)
    return jnp.where(col <= row, value, 0.0)


def kernel(
    levels,
    ring_size,
    matrix,
    v1,
    f1,
    u1,
    g1,
    v2,
    f2,
    u2,
    g2,
    x,
    leafs,
    trees,
    far_mixers,
    tops,
    far_folds,
    folds,
    far_tops,
    passed,
    op_v,
    op_vt,
    op_f,
    op_u,
    op_ut,
    op_g,
    op_far,
    load_sem,
    x_sem,
    ring_send,
    ring_recv,
    fold_send,
    fold_recv,
    top_send,
    top_recv,
    pass_send,
    mixer_send,
    mixer_recv,
):
    rows, columns = x.shape
    chunks = columns // LANES
    pairs = columns // PAIR
    width = trees.shape[1]
    share = width // ring_size
    half = ring_size // 2

    d = lax.axis_index("row")
    k = lax.axis_index("col")
    right = lax.rem(k + 1, ring_size)
    left = lax.rem(k + ring_size - 1, ring_size)
    steps = jnp.int32(0)
    reach = jnp.int32(1)
    for i in range(levels):
        one = jnp.where(lax.rem(d, 2 ** (i + 1)) == 0, 1, 0)
        steps = steps + one
        reach = reach + one * 2**i
    not_root = d != 0
    parent = d - reach
    hands_on = jnp.int32(0)
    handed = jnp.int32(0)
    for i in CHAINED:
        if i < levels:
            hands_on = hands_on + jnp.where(lax.rem(d, 2 ** (i + 1)) == 2 ** (i - 1), 1, 0)
            handed = handed + jnp.where(lax.rem(d, 2 ** (i + 1)) == 2**i, 1, 0)
    before_me = d - reach // 2
    after_me = d + reach

    own = pl.ds(pl.multiple_of(k * share, share), share)
    loads = []
    for p, (v, f, u, g) in enumerate(((v1, f1, u1, g1), (v2, f2, u2, g2))):
        places = (
            (v, leafs.at[p, own, pl.ds(0, rows)]),
            (f, leafs.at[p, own, pl.ds(rows, width)]),
            (u, trees.at[p, own, pl.ds(0, width)]),
            (g, trees.at[p, own, pl.ds(width, width)]),
        )
        for i, (source, place) in enumerate(places):
            loads.append(pltpu.make_async_copy(source, place, load_sem.at[p, i]))
    x_load = pltpu.make_async_copy(matrix, x, x_sem)

    barrier = pltpu.get_barrier_semaphore()

    def greet(row, col):
        pl.semaphore_signal(barrier, inc=1, device_id=(row, col), device_id_type=MESH)

    greet(d, left)
    greet(d, right)

    def greet_lower(i, stride):
        greet(d + stride, k)
        return stride * 2

    lax.fori_loop(0, steps, greet_lower, jnp.int32(1))

    @pl.when(not_root)
    def _():
        greet(parent, k)

    @pl.when(hands_on > 0)
    def _():
        greet(after_me, k)

    @pl.when(handed > 0)
    def _():
        greet(before_me, k)

    for copy in loads[:4] + [x_load] + loads[4:]:
        copy.start()
    with jax.named_scope("barrier"):
        pl.semaphore_wait(
            barrier, 2 + steps + jnp.where(not_root, 1, 0) + hands_on + handed
        )

    starts = ((0, 2 * LANES), (2 * LANES, rows - LANES), (0, width), (width, width))

    def hops(piece, way):
        return half if piece % 2 == way else half - 1

    def ring_copy(p, piece, way, hop, sent):
        back = hop - 1 if sent else hop
        shard = lax.rem(k + (ring_size - back if way == 0 else back), ring_size)
        row = pl.ds(pl.multiple_of(shard * share, share), share)
        start, size = starts[piece]
        if piece < 2:
            first = ((shard * share) // LANES) * LANES
            lanes = pl.ds(pl.multiple_of(first + start, LANES), size)
            ref = leafs.at[p, row, lanes]
        else:
            ref = trees.at[p, row, pl.ds(start, size)]
        return pltpu.make_async_remote_copy(
            src_ref=ref,
            dst_ref=ref,
            send_sem=ring_send.at[p, piece, way, hop - 1],
            recv_sem=ring_recv.at[p, piece, way, hop - 1],
            device_id=(d, right if way == 0 else left),
            device_id_type=MESH,
        )

    def relay(p, hop):
        for piece in range(4):
            for way in range(2):
                if hop <= hops(piece, way):
                    if hop > 1:
                        ring_copy(p, piece, way, hop - 1, False).wait_recv()
                    ring_copy(p, piece, way, hop, True).start()

    def gathered(p, pieces):
        for piece in pieces:
            for way in range(2):
                if hops(piece, way) > 0:
                    ring_copy(p, piece, way, hops(piece, way), False).wait_recv()

    def top_copy(p, level, c, stride):
        return pltpu.make_async_remote_copy(
            src_ref=tops.at[p, level, c],
            dst_ref=far_tops.at[p, c],
            send_sem=top_send.at[p, level, c],
            recv_sem=top_recv.at[p, c],
            device_id=(d + stride, k),
            device_id_type=MESH,
        )

    def pass_copy(p, c):
        return pltpu.make_async_remote_copy(
            src_ref=passed.at[p, c],
            dst_ref=far_tops.at[p, c],
            send_sem=pass_send.at[p, c],
            recv_sem=top_recv.at[p, c],
            device_id=(after_me, k),
            device_id_type=MESH,
        )

    def sends_top(level):
        sends = level < steps
        for i in CHAINED:
            sends = sends & (level != i)
        return sends

    def fold_copy(p, c, level):
        return pltpu.make_async_remote_copy(
            src_ref=folds.at[p, c],
            dst_ref=far_folds.at[p, level, c],
            send_sem=fold_send.at[p, c],
            recv_sem=fold_recv.at[p, level, c],
            device_id=(parent, k),
            device_id_type=MESH,
        )

    def mixer_copy(p, level):
        return pltpu.make_async_remote_copy(
            src_ref=trees.at[p, :, pl.ds(width, width)],
            dst_ref=far_mixers.at[p, level],
            send_sem=mixer_send.at[p],
            recv_sem=mixer_recv.at[p, level],
            device_id=(parent, k),
            device_id_type=MESH,
        )

    late = steps == levels - 1

    def fold(p, c):
        folds[p, c] = times(op_ut, tops[p, steps, c])

        @pl.when((p > 0) | jnp.logical_not(late))
        def _():
            fold_copy(p, c, steps).start()

    def chunks_of(pair):
        return range(pair * (PAIR // LANES), (pair + 1) * (PAIR // LANES))

    def each_chunk(body):
        def step(c, carry):
            body(c)
            return carry

        lax.fori_loop(0, chunks, step, 0)

    def prepare_leaf(p, offset):
        raw = leafs[p, :, pl.ds(0, rows)]
        row = lax.broadcasted_iota(jnp.int32, raw.shape, 1) - offset
        col = lax.broadcasted_iota(jnp.int32, raw.shape, 0)
        vectors = jnp.where(row > col, raw, jnp.where(row == col, 1.0, 0.0))
        op_vt[...] = left_operand(vectors)
        op_v[...] = left_operand(vectors.T)
        op_f[...] = left_operand(lower_triangle(leafs[p, :, pl.ds(rows, width)]))

    def prepare_tree(p):
        merge = lower_triangle(trees[p, :, pl.ds(0, width)])
        op_ut[...] = left_operand(merge)
        op_u[...] = left_operand(merge.T)
        op_g[...] = left_operand(lower_triangle(trees[p, :, pl.ds(width, width)]))

    def panel(p, offset):
        block = pl.ds(pl.multiple_of(offset, width), width)
        with jax.named_scope("wait_vectors"):
            gathered(p, (0, 1))
        with jax.named_scope("prepare_leaf"):
            prepare_leaf(p, offset)
        if p == 0:
            x_load.wait()

        for pair in range(pairs):
            with jax.named_scope("leaf"):
                lanes = pl.ds(pair * PAIR, PAIR)
                before = x[:, lanes]
                mixed = times(op_f, times(op_vt, before))
                x[:, lanes] = before - times(op_v, mixed)
                for c in chunks_of(pair):
                    tops[p, 0, c] = x[block, pl.ds(c * LANES, LANES)]

                    @pl.when(steps > 0)
                    def _():
                        top_copy(p, 0, c, 1).start()

            if pair == 0:
                with jax.named_scope("wait_merges"):
                    gathered(p, (2, 3))

                @pl.when(not_root)
                def _():
                    mixer_copy(p, steps).start()

        with jax.named_scope("prepare_tree"):
            prepare_tree(p)

        @pl.when(steps == 0)
        def _():
            with jax.named_scope("first_fold"):
                each_chunk(functools.partial(fold, p))

        def level_step(level, stride):
            prepare_far(p, level, 0)
            each_chunk(functools.partial(upper, p, level, stride, 0))
            if p == 0:
                for hop in range(2, half + 1):

                    @pl.when(level == hop - 2)
                    def _():
                        with jax.named_scope("relay"):
                            relay(1, hop)

            return stride * 2

        near = max(levels - 3, 0)
        lax.fori_loop(0, jnp.minimum(steps, near), level_step, jnp.int32(1))

        @pl.when(steps > near)
        def _():
            prepare_far(p, near, 0)

            @pl.when(steps > near + 1)
            def _():
                prepare_far(p, near + 1, 1)

            def two_levels(c):
                upper(p, near, 2**near, 0, c)

                @pl.when(steps > near + 1)
                def _():
                    upper(p, near + 1, 2 ** (near + 1), 1, c)

            each_chunk(two_levels)

    def prepare_far(p, level, slot):
        with jax.named_scope("wait_mixer"):
            mixer_copy(p, level).wait_recv()
        op_far[slot] = left_operand(lower_triangle(far_mixers[p, level]))

    def upper(p, level, stride, slot, c):
        with jax.named_scope("wait_fold"):
            fold_copy(p, c, level).wait_recv()
        before = tops[p, level, c]
        weight = times(op_far.at[slot], before + far_folds[p, level, c])
        tops[p, level + 1, c] = before - weight

        @pl.when(sends_top(level + 1))
        def _():
            top_copy(p, level + 1, c, stride * 2).start()

        @pl.when((level + 1 == steps) & not_root)
        def _():
            fold(p, c)

    def lower(p):
        for c in range(chunks):
            with jax.named_scope("wait_top"):
                top_copy(p, 0, c, 0).wait_recv()
            upper_rows = far_tops[p, c]
            weight = times(op_g, upper_rows + folds[p, c])

            @pl.when(hands_on > 0)
            def _():
                passed[p, c] = upper_rows - weight
                pass_copy(p, c).start()

            x[pl.ds(0, width), pl.ds(c * LANES, LANES)] = (
                tops[p, steps, c] - times(op_u, weight)
            )

    def root(p, first):
        last = levels - 1
        prepare_far(p, last, 0)
        for c in range(chunks):
            upper(p, last, 2**last, 0, c)
            x[pl.ds(first, width), pl.ds(c * LANES, LANES)] = tops[p, levels, c]

    for copy in loads[:4]:
        copy.wait()
    for hop in range(1, half + 1):
        with jax.named_scope("ring"):
            relay(0, hop)
    for copy in loads[4:]:
        copy.wait()
    relay(1, 1)
    panel(0, jnp.int32(0))

    @pl.when(late)
    def _():
        each_chunk(lambda c: fold_copy(0, c, steps).start())

    near = max(levels - 3, 0)
    for hop in range(2, min(half, near + 2) + 1):

        @pl.when(steps == hop - 2)
        def _():
            with jax.named_scope("relay"):
                relay(1, hop)

    @pl.when(not_root)
    def _():
        lower(0)

    for hop in range(2, half + 1):
        due = jnp.minimum(steps, near) <= hop - 2
        if hop <= near + 2:
            due = due & (steps != hop - 2)

        @pl.when(due)
        def _():
            with jax.named_scope("relay"):
                relay(1, hop)

    panel(1, jnp.where(not_root, 0, width))

    @pl.when(not_root)
    def _():
        lower(1)

    @pl.when(d == 0)
    def _():
        root(0, 0)
        root(1, width)

    for p in range(2):
        for piece in range(4):
            for way in range(2):
                for hop in range(1, hops(piece, way) + 1):
                    ring_copy(p, piece, way, hop, True).wait_send()

        def sent_tops(level, carry):
            @pl.when(sends_top(level))
            def _():
                each_chunk(lambda c: top_copy(p, level, c, 0).wait_send())

            return carry

        lax.fori_loop(0, steps, sent_tops, 0)

        @pl.when(hands_on > 0)
        def _():
            each_chunk(lambda c: pass_copy(p, c).wait_send())

        @pl.when(not_root)
        def _():
            mixer_copy(p, steps).wait_send()
            each_chunk(lambda c: fold_copy(p, c, steps).wait_send())


def local(levels, ring_size, matrix, *reflectors):
    rows, cols = matrix.shape
    turned = [r.T for r in reflectors]
    width = turned[1].shape[1]
    chunks = cols // LANES
    half = ring_size // 2
    vmem, dma = pltpu.VMEM, pltpu.SemaphoreType.DMA
    anywhere = pl.BlockSpec(memory_space=pltpu.HBM)
    tile = (chunks, width, LANES)
    flops = 2 * 3 * 2 * cols * width * (3 * rows + 9 * width)
    arrays = (matrix, *turned)
    return pl.pallas_call(
        functools.partial(kernel, levels, ring_size),
        out_shape=jax.ShapeDtypeStruct(matrix.shape, matrix.dtype),
        in_specs=[anywhere] * 9,
        out_specs=pl.BlockSpec(memory_space=pltpu.VMEM),
        scratch_shapes=[
            vmem((2, width, rows + width), F32),
            vmem((2, width, 2 * width), F32),
            vmem((2, levels, width, width), F32),
            vmem((2, levels + 1, *tile), F32),
            vmem((2, levels, *tile), F32),
            vmem((2, *tile), F32),
            vmem((2, *tile), F32),
            vmem((2, *tile), F32),
            vmem((rows, 3 * width), BF16),
            vmem((width, 3 * rows), BF16),
            vmem((width, 3 * width), BF16),
            vmem((width, 3 * width), BF16),
            vmem((width, 3 * width), BF16),
            vmem((width, 3 * width), BF16),
            vmem((2, width, 3 * width), BF16),
            dma((2, 4)),
            dma(()),
            dma((2, 4, 2, half)),
            dma((2, 4, 2, half)),
            dma((2, chunks)),
            dma((2, levels, chunks)),
            dma((2, levels, chunks)),
            dma((2, chunks)),
            dma((2, chunks)),
            dma((2,)),
            dma((2, levels)),
        ],
        compiler_params=pltpu.CompilerParams(
            collective_id=0, has_side_effects=True, vmem_limit_bytes=50_331_648
        ),
        cost_estimate=pl.CostEstimate(
            flops=flops, bytes_accessed=8 * rows * cols, transcendentals=0
        ),
        name="tree_update",
    )(*(pltpu.with_memory_space_constraint(a, pltpu.HBM) for a in arrays))


def solution(mesh):
    levels = mesh.shape["row"].bit_length() - 1
    placed = P("row", "col")
    return jax.shard_map(
        functools.partial(local, levels, mesh.shape["col"]),
        mesh=mesh,
        in_specs=(placed,) * 9,
        out_specs=placed,
        check_vma=False,
    )
```

```python
import functools

import jax
import jax.numpy as jnp
from jax import lax
from jax.experimental import pallas as pl
from jax.experimental.pallas import tpu as pltpu
from jax.sharding import PartitionSpec as P

LANES = 128
PAIR = 256
CHAINED = (2, 4, 5)
MESH = pl.DeviceIdType.MESH
F32 = jnp.float32
BF16 = jnp.bfloat16


def halves(value):
    high = value.astype(BF16)
    return high, (value - high.astype(F32)).astype(BF16)


def left_operand(value):
    high, low = halves(value)
    return jnp.concatenate([high, high, low], axis=1)


def times(operator, value):
    high, low = halves(value)
    right = jnp.concatenate([high, low, high], axis=0)
    return jnp.dot(operator[...], right, preferred_element_type=F32)


def lower_triangle(value):
    row = lax.broadcasted_iota(jnp.int32, value.shape, 0)
    col = lax.broadcasted_iota(jnp.int32, value.shape, 1)
    return jnp.where(col <= row, value, 0.0)


def kernel(
    levels,
    ring_size,
    matrix,
    v1,
    f1,
    u1,
    g1,
    v2,
    f2,
    u2,
    g2,
    x,
    leafs,
    trees,
    far_mixers,
    tops,
    far_folds,
    folds,
    far_tops,
    passed,
    op_v,
    op_vt,
    op_f,
    op_u,
    op_ut,
    op_g,
    op_far,
    load_sem,
    x_sem,
    ring_send,
    ring_recv,
    fold_send,
    fold_recv,
    top_send,
    top_recv,
    pass_send,
    mixer_send,
    mixer_recv,
):
    rows, columns = x.shape
    chunks = columns // LANES
    pairs = columns // PAIR
    width = trees.shape[1]
    share = width // ring_size
    half = ring_size // 2

    d = lax.axis_index("row")
    k = lax.axis_index("col")
    right = lax.rem(k + 1, ring_size)
    left = lax.rem(k + ring_size - 1, ring_size)
    steps = jnp.int32(0)
    reach = jnp.int32(1)
    for i in range(levels):
        one = jnp.where(lax.rem(d, 2 ** (i + 1)) == 0, 1, 0)
        steps = steps + one
        reach = reach + one * 2**i
    not_root = d != 0
    parent = d - reach
    hands_on = jnp.int32(0)
    handed = jnp.int32(0)
    for i in CHAINED:
        if i < levels:
            hands_on = hands_on + jnp.where(lax.rem(d, 2 ** (i + 1)) == 2 ** (i - 1), 1, 0)
            handed = handed + jnp.where(lax.rem(d, 2 ** (i + 1)) == 2**i, 1, 0)
    before_me = d - reach // 2
    after_me = d + reach

    own = pl.ds(pl.multiple_of(k * share, share), share)
    loads = []
    for p, (v, f, u, g) in enumerate(((v1, f1, u1, g1), (v2, f2, u2, g2))):
        places = (
            (v, leafs.at[p, own, pl.ds(0, rows)]),
            (f, leafs.at[p, own, pl.ds(rows, width)]),
            (u, trees.at[p, own, pl.ds(0, width)]),
            (g, trees.at[p, own, pl.ds(width, width)]),
        )
        for i, (source, place) in enumerate(places):
            loads.append(pltpu.make_async_copy(source, place, load_sem.at[p, i]))
    x_load = pltpu.make_async_copy(matrix, x, x_sem)

    barrier = pltpu.get_barrier_semaphore()

    def greet(row, col):
        pl.semaphore_signal(barrier, inc=1, device_id=(row, col), device_id_type=MESH)

    greet(d, left)
    greet(d, right)

    def greet_lower(i, stride):
        greet(d + stride, k)
        return stride * 2

    lax.fori_loop(0, steps, greet_lower, jnp.int32(1))

    @pl.when(not_root)
    def _():
        greet(parent, k)

    @pl.when(hands_on > 0)
    def _():
        greet(after_me, k)

    @pl.when(handed > 0)
    def _():
        greet(before_me, k)

    for copy in loads[:4] + [x_load] + loads[4:]:
        copy.start()
    with jax.named_scope("barrier"):
        pl.semaphore_wait(
            barrier, 2 + steps + jnp.where(not_root, 1, 0) + hands_on + handed
        )

    starts = ((0, 2 * LANES), (2 * LANES, rows - LANES), (0, width), (width, width))

    def hops(piece, way):
        return half if piece % 2 == way else half - 1

    def ring_copy(p, piece, way, hop, sent):
        back = hop - 1 if sent else hop
        shard = lax.rem(k + (ring_size - back if way == 0 else back), ring_size)
        row = pl.ds(pl.multiple_of(shard * share, share), share)
        start, size = starts[piece]
        if piece < 2:
            first = ((shard * share) // LANES) * LANES
            lanes = pl.ds(pl.multiple_of(first + start, LANES), size)
            ref = leafs.at[p, row, lanes]
        else:
            ref = trees.at[p, row, pl.ds(start, size)]
        return pltpu.make_async_remote_copy(
            src_ref=ref,
            dst_ref=ref,
            send_sem=ring_send.at[p, piece, way, hop - 1],
            recv_sem=ring_recv.at[p, piece, way, hop - 1],
            device_id=(d, right if way == 0 else left),
            device_id_type=MESH,
        )

    def relay(p, hop):
        for piece in range(4):
            for way in range(2):
                if hop <= hops(piece, way):
                    if hop > 1:
                        ring_copy(p, piece, way, hop - 1, False).wait_recv()
                    ring_copy(p, piece, way, hop, True).start()

    def gathered(p, pieces):
        for piece in pieces:
            for way in range(2):
                if hops(piece, way) > 0:
                    ring_copy(p, piece, way, hops(piece, way), False).wait_recv()

    def top_copy(p, level, c, stride):
        return pltpu.make_async_remote_copy(
            src_ref=tops.at[p, level, c],
            dst_ref=far_tops.at[p, c],
            send_sem=top_send.at[p, level, c],
            recv_sem=top_recv.at[p, c],
            device_id=(d + stride, k),
            device_id_type=MESH,
        )

    def pass_copy(p, c):
        return pltpu.make_async_remote_copy(
            src_ref=passed.at[p, c],
            dst_ref=far_tops.at[p, c],
            send_sem=pass_send.at[p, c],
            recv_sem=top_recv.at[p, c],
            device_id=(after_me, k),
            device_id_type=MESH,
        )

    def sends_top(level):
        sends = level < steps
        for i in CHAINED:
            sends = sends & (level != i)
        return sends

    def fold_copy(p, c, level):
        return pltpu.make_async_remote_copy(
            src_ref=folds.at[p, c],
            dst_ref=far_folds.at[p, level, c],
            send_sem=fold_send.at[p, c],
            recv_sem=fold_recv.at[p, level, c],
            device_id=(parent, k),
            device_id_type=MESH,
        )

    def mixer_copy(p, level):
        return pltpu.make_async_remote_copy(
            src_ref=trees.at[p, :, pl.ds(width, width)],
            dst_ref=far_mixers.at[p, level],
            send_sem=mixer_send.at[p],
            recv_sem=mixer_recv.at[p, level],
            device_id=(parent, k),
            device_id_type=MESH,
        )

    late = steps == levels - 1

    def fold(p, c):
        folds[p, c] = times(op_ut, tops[p, steps, c])

        @pl.when((p > 0) | jnp.logical_not(late))
        def _():
            fold_copy(p, c, steps).start()

    def chunks_of(pair):
        return range(pair * (PAIR // LANES), (pair + 1) * (PAIR // LANES))

    def each_chunk(body):
        def step(c, carry):
            body(c)
            return carry

        lax.fori_loop(0, chunks, step, 0)

    def prepare_leaf(p, offset):
        raw = leafs[p, :, pl.ds(0, rows)]
        row = lax.broadcasted_iota(jnp.int32, raw.shape, 1) - offset
        col = lax.broadcasted_iota(jnp.int32, raw.shape, 0)
        vectors = jnp.where(row > col, raw, jnp.where(row == col, 1.0, 0.0))
        op_vt[...] = left_operand(vectors)
        op_v[...] = left_operand(vectors.T)
        op_f[...] = left_operand(lower_triangle(leafs[p, :, pl.ds(rows, width)]))

    def prepare_tree(p):
        merge = lower_triangle(trees[p, :, pl.ds(0, width)])
        op_ut[...] = left_operand(merge)
        op_u[...] = left_operand(merge.T)
        op_g[...] = left_operand(lower_triangle(trees[p, :, pl.ds(width, width)]))

    def panel(p, offset):
        block = pl.ds(pl.multiple_of(offset, width), width)
        with jax.named_scope("wait_vectors"):
            gathered(p, (0, 1))
        with jax.named_scope("prepare_leaf"):
            prepare_leaf(p, offset)
        if p == 0:
            x_load.wait()

        for pair in range(pairs):
            with jax.named_scope("leaf"):
                lanes = pl.ds(pair * PAIR, PAIR)
                before = x[:, lanes]
                mixed = times(op_f, times(op_vt, before))
                x[:, lanes] = before - times(op_v, mixed)
                for c in chunks_of(pair):
                    tops[p, 0, c] = x[block, pl.ds(c * LANES, LANES)]

                    @pl.when(steps > 0)
                    def _():
                        top_copy(p, 0, c, 1).start()

            if pair == 0:
                with jax.named_scope("wait_merges"):
                    gathered(p, (2, 3))

                @pl.when(not_root)
                def _():
                    mixer_copy(p, steps).start()

        with jax.named_scope("prepare_tree"):
            prepare_tree(p)

        @pl.when(steps == 0)
        def _():
            with jax.named_scope("first_fold"):
                each_chunk(functools.partial(fold, p))

        def level_step(level, stride):
            prepare_far(p, level, 0)
            each_chunk(functools.partial(upper, p, level, stride, 0))
            if p == 0:
                for hop in range(2, half + 1):

                    @pl.when(level == hop - 2)
                    def _():
                        with jax.named_scope("relay"):
                            relay(1, hop)

            return stride * 2

        near = max(levels - 3, 0)
        lax.fori_loop(0, jnp.minimum(steps, near), level_step, jnp.int32(1))

        @pl.when(steps > near)
        def _():
            prepare_far(p, near, 0)

            @pl.when(steps > near + 1)
            def _():
                prepare_far(p, near + 1, 1)

            def two_levels(c):
                upper(p, near, 2**near, 0, c)

                @pl.when(steps > near + 1)
                def _():
                    upper(p, near + 1, 2 ** (near + 1), 1, c)

            each_chunk(two_levels)

    def prepare_far(p, level, slot):
        with jax.named_scope("wait_mixer"):
            mixer_copy(p, level).wait_recv()
        op_far[slot] = left_operand(lower_triangle(far_mixers[p, level]))

    def upper(p, level, stride, slot, c):
        with jax.named_scope("wait_fold"):
            fold_copy(p, c, level).wait_recv()
        before = tops[p, level, c]
        weight = times(op_far.at[slot], before + far_folds[p, level, c])
        tops[p, level + 1, c] = before - weight

        @pl.when(sends_top(level + 1))
        def _():
            top_copy(p, level + 1, c, stride * 2).start()

        @pl.when((level + 1 == steps) & not_root)
        def _():
            fold(p, c)

    def lower(p):
        for c in range(chunks):
            with jax.named_scope("wait_top"):
                top_copy(p, 0, c, 0).wait_recv()
            upper_rows = far_tops[p, c]
            weight = times(op_g, upper_rows + folds[p, c])

            @pl.when(hands_on > 0)
            def _():
                passed[p, c] = upper_rows - weight
                pass_copy(p, c).start()

            x[pl.ds(0, width), pl.ds(c * LANES, LANES)] = (
                tops[p, steps, c] - times(op_u, weight)
            )

    def root(p, first):
        last = levels - 1
        prepare_far(p, last, 0)
        for c in range(chunks):
            upper(p, last, 2**last, 0, c)
            x[pl.ds(first, width), pl.ds(c * LANES, LANES)] = tops[p, levels, c]

    def sent(p):
        def sent_tops(level, carry):
            @pl.when(sends_top(level))
            def _():
                each_chunk(lambda c: top_copy(p, level, c, 0).wait_send())

            return carry

        lax.fori_loop(0, steps, sent_tops, 0)

        @pl.when(hands_on > 0)
        def _():
            each_chunk(lambda c: pass_copy(p, c).wait_send())

        @pl.when(not_root)
        def _():
            mixer_copy(p, steps).wait_send()
            each_chunk(lambda c: fold_copy(p, c, steps).wait_send())

    for copy in loads[:4]:
        copy.wait()
    for hop in range(1, half + 1):
        with jax.named_scope("ring"):
            relay(0, hop)
    for copy in loads[4:]:
        copy.wait()
    relay(1, 1)
    panel(0, jnp.int32(0))

    @pl.when(late)
    def _():
        each_chunk(lambda c: fold_copy(0, c, steps).start())

    near = max(levels - 3, 0)
    for hop in range(2, min(half, near + 2) + 1):

        @pl.when(steps == hop - 2)
        def _():
            with jax.named_scope("relay"):
                relay(1, hop)

    @pl.when(not_root)
    def _():
        lower(0)

    for hop in range(2, half + 1):
        due = jnp.minimum(steps, near) <= hop - 2
        if hop <= near + 2:
            due = due & (steps != hop - 2)

        @pl.when(due)
        def _():
            with jax.named_scope("relay"):
                relay(1, hop)

    panel(1, jnp.where(not_root, 0, width))

    for p in range(2):
        for piece in range(4):
            for way in range(2):
                for hop in range(1, hops(piece, way) + 1):
                    ring_copy(p, piece, way, hop, True).wait_send()
    sent(0)

    @pl.when(not_root)
    def _():
        lower(1)

    @pl.when(d == 0)
    def _():
        root(0, 0)
        root(1, width)

    sent(1)


def local(levels, ring_size, matrix, *reflectors):
    rows, cols = matrix.shape
    turned = [r.T for r in reflectors]
    width = turned[1].shape[1]
    chunks = cols // LANES
    half = ring_size // 2
    vmem, dma = pltpu.VMEM, pltpu.SemaphoreType.DMA
    anywhere = pl.BlockSpec(memory_space=pltpu.HBM)
    tile = (chunks, width, LANES)
    flops = 2 * 3 * 2 * cols * width * (3 * rows + 9 * width)
    arrays = (matrix, *turned)
    return pl.pallas_call(
        functools.partial(kernel, levels, ring_size),
        out_shape=jax.ShapeDtypeStruct(matrix.shape, matrix.dtype),
        in_specs=[anywhere] * 9,
        out_specs=pl.BlockSpec(memory_space=pltpu.VMEM),
        scratch_shapes=[
            vmem((2, width, rows + width), F32),
            vmem((2, width, 2 * width), F32),
            vmem((2, levels, width, width), F32),
            vmem((2, levels + 1, *tile), F32),
            vmem((2, levels, *tile), F32),
            vmem((2, *tile), F32),
            vmem((2, *tile), F32),
            vmem((2, *tile), F32),
            vmem((rows, 3 * width), BF16),
            vmem((width, 3 * rows), BF16),
            vmem((width, 3 * width), BF16),
            vmem((width, 3 * width), BF16),
            vmem((width, 3 * width), BF16),
            vmem((width, 3 * width), BF16),
            vmem((2, width, 3 * width), BF16),
            dma((2, 4)),
            dma(()),
            dma((2, 4, 2, half)),
            dma((2, 4, 2, half)),
            dma((2, chunks)),
            dma((2, levels, chunks)),
            dma((2, levels, chunks)),
            dma((2, chunks)),
            dma((2, chunks)),
            dma((2,)),
            dma((2, levels)),
        ],
        compiler_params=pltpu.CompilerParams(
            collective_id=0, has_side_effects=True, vmem_limit_bytes=50_331_648
        ),
        cost_estimate=pl.CostEstimate(
            flops=flops, bytes_accessed=8 * rows * cols, transcendentals=0
        ),
        name="tree_update",
    )(*(pltpu.with_memory_space_constraint(a, pltpu.HBM) for a in arrays))


def solution(mesh):
    levels = mesh.shape["row"].bit_length() - 1
    placed = P("row", "col")
    return jax.shard_map(
        functools.partial(local, levels, mesh.shape["col"]),
        mesh=mesh,
        in_specs=(placed,) * 9,
        out_specs=placed,
        check_vma=False,
    )
```
